32 devices in a mesh: gx: 4 (over z), gy: 4 (over y, core), gz: 2 (over x).
Axes of the slice: x: 2, y: 2, z: 4, core: 2. Of those that a mesh axis runs over, the one named last changes fastest.
Arguments:
- gas_position: float32 [3, 131072], P(None, ('gx', 'gy', 'gz')), may hold values from 0 to 1
- gas_mass: float32 [131072], P(('gx', 'gy', 'gz')), may hold values from 0.3 to 3
- gas_smoothing: float32 [131072], P(('gx', 'gy', 'gz')), may hold values from 0.5 to 1.5
- leaf_counts: int32 [1024], P(('gx', 'gy', 'gz')), may hold values from 64 to 128
- ghost_lists: int32 [32, 4, 2], P(('gx', 'gy', 'gz')), may hold values from 0 to 31, as said below
- star_position: float32 [3, 65536], P(None, ('gx', 'gy', 'gz')), may hold values from 0 to 1
- star_energy: float32 [65536], P(('gx', 'gy', 'gz')), may hold values from 0.1 to 10
- star_momentum: float32 [3, 65536], P(None, ('gx', 'gy', 'gz')), may hold values from -6 to 6
- block_counts: int32 [512], P(('gx', 'gy', 'gz')), may hold values from 1 to 128
- block_owners: int32 [512, 1], P(('gx', 'gy', 'gz')), may hold values from 0 to 7; in each aligned block of 16 rows (0 to 15, 16 to 31, ...) at most 3 rows name the same one
- block_leaves: int32 [512], P(('gx', 'gy', 'gz')), may hold values from 0 to 31
Outputs:
- accel: float32 [3, 131072], P(None, ('gx', 'gy', 'gz'))
- deposit: float32 [4, 131072], P(None, ('gx', 'gy', 'gz'))
The draws below stay inside these ranges and needn't reach their ends.
Inputs may be any that keep to these rules, and one draw needn't show every extreme that they name: `ghost_lists`: each of the four lists of a device names 2 different leaves. `block_owners`: among the 16 star blocks of one device, no owner is named more than 3 times, and in some devices one owner is named exactly 3 times.
All inputs are finite; a program needn't handle non-finite values.
Results may differ from the reference program's by a relative error of at most 0.00015.
Values sent between devices are 32-bit elements; how exact they have to be, the bound alone decides.
A program may use at most 64 MiB of HBM per device.

```python
import math
import jax
import jax.numpy as jnp
import numpy as np
from jax import lax

LEAVES = 32
LEAF_SLOTS = 128
GHOSTS = 2
STARS_BLOCK = 128
SLOTS = 3
OWNERS = 8
BLOCKS = 16
PARTICLES = 131072
STAR_BLOCKS = 512
STARS = 65536
N_GX = 4
N_GY = 4
N_GZ = 2
DEVICES = 32


def draw_ghost_lists(key, part):
    keys = jax.random.split(jax.random.fold_in(key, 17), DEVICES * 4)
    picks = jax.vmap(lambda one_key: jax.random.permutation(one_key, LEAVES)[:GHOSTS])(keys)
    return picks.reshape(DEVICES, 4, GHOSTS).astype(jnp.int32)


def set_ends(values, rng, least, high):
    dims = values.shape
    place = [jax.random.randint(jax.random.fold_in(rng, axis), (), 0, dims[axis]) for axis in range(len(dims))]
    values = values.at[tuple(place)].set(least)
    longest = dims.index(max(dims))
    place[longest] = (place[longest] + 1) % dims[longest]
    return values.at[tuple(place)].set(high)


def levels(key, dims, cuts, low, high):
    factor_of, own = 1.0, jax.random.fold_in(key, 6)
    for dim, parts in cuts:
        draws = jnp.exp(jax.random.uniform(jax.random.fold_in(own, dim), (parts,), jnp.float32, low / len(cuts), high / len(cuts)))
        factor_of = factor_of * jnp.repeat(draws, dims[dim] // parts).reshape([-1 if axis == dim else 1 for axis in range(len(dims))])
    return factor_of


def assign_block(stream_key, own, number, rows, count, top, reach, lean):
    ranking = jax.random.permutation(stream_key, count)
    heavy_load, ordinary = portions_of(count, rows * top, reach, lean, True), portions_of(count, rows * top, reach, lean, False)
    places = jnp.arange(count)

    def named(sizes, turn):
        used = int((sizes > 0).sum())
        fixed = max(1, used // 4)
        shifted = fixed + (places - fixed + turn * (used - fixed)) % max(1, count - fixed)
        return jnp.zeros((count,), jnp.int32).at[ranking[jnp.where(places < fixed, places, shifted)]].set(jnp.asarray(sizes, jnp.int32))

    sizes = jnp.where(number % 4 == 0, named(heavy_load, number // 4), named(ordinary, number - number // 4 - 1))
    mixed = jax.random.permutation(jax.random.fold_in(own, 3), count)
    giver, receiver = mixed[0:count // 2 * 2:2], mixed[1:count // 2 * 2:2]
    room = jnp.minimum(sizes[giver] - 1, reach - sizes[receiver]) // 2
    room = jnp.where((giver == ranking[0]) | (receiver == ranking[0]) | (sizes[receiver] == 0), 0, jnp.maximum(room, 0))
    shifted = jax.random.randint(jax.random.fold_in(own, 4), (count // 2,), 0, 1 << 20) % (room + 1)
    sizes = sizes.at[giver].add(-shifted).at[receiver].add(shifted)
    members = jnp.searchsorted(jnp.cumsum(sizes), jnp.arange(rows * top), side="right").astype(jnp.int32)
    table = members.reshape(top, rows).T
    table = table[jax.random.permutation(jax.random.fold_in(own, 1), rows)]
    turn = jax.random.randint(jax.random.fold_in(own, 2), (rows, 1), 0, top)
    return jnp.take_along_axis(table, (jnp.arange(top)[None, :] + turn) % top, axis=1)


def portions_of(count, total, reach, lean, full):
    weights = [(1 << 20) // math.isqrt(rank ** lean) + 1 for rank in range(1, count + 1)]
    largest = reach if full else min(reach, max(-(-total // count), total * weights[0] // sum(weights)))
    least = 1 if total - largest >= count - 1 else 0
    counts, spare = [largest] + [least] * (count - 1), total - largest - least * (count - 1)
    while spare > 0:
        movable = [i for i in range(1, count) if counts[i] < largest] or [i for i in range(1, count) if counts[i] < reach]
        whole, budget = sum([weights[i] for i in movable]), spare
        for i in movable:
            addition = min(reach - counts[i], max(1, budget * weights[i] // whole), spare)
            counts[i] = counts[i] + addition
            spare = spare - addition
    return np.array(counts)


def gaussian(own_key, dims, scale, limit, cuts=(), kind=jnp.bfloat16):
    gain = levels(own_key, dims, cuts, -0.22, 0.18) if cuts else 1.0
    entries = jax.random.normal(own_key, dims, jnp.float32) * scale * gain
    return jnp.minimum(jnp.maximum(entries, -limit), limit).astype(kind)


def setup_inputs(seed: int = 0) -> dict:
    streams_of = jax.random.split(jax.random.key(seed), 12)
    gas_position = jnp.clip(1.0 * jax.random.uniform(streams_of[0], (3, PARTICLES), jnp.float32) ** levels(streams_of[0], (3, PARTICLES), ((1, 32),), -0.2, 0.2), 0.0, 1.0)
    gas_mass = jnp.clip(jnp.exp(math.log(3.0) - 2.3025851 * jax.random.uniform(streams_of[1], (PARTICLES,), jnp.float32) ** levels(streams_of[1], (PARTICLES,), ((0, 32),), -0.2, 0.2)), 0.3, 3.0)
    gas_smoothing = jnp.clip(jnp.exp(math.log(1.5) - 1.0986123 * jax.random.uniform(streams_of[2], (PARTICLES,), jnp.float32) ** levels(streams_of[2], (PARTICLES,), ((0, 32),), -0.2, 0.2)), 0.5, 1.5)
    leaf_counts = set_ends(jax.random.randint(streams_of[3], (DEVICES * LEAVES,), LEAF_SLOTS // 2, LEAF_SLOTS + 1), jax.random.fold_in(streams_of[3], 1), LEAF_SLOTS // 2, LEAF_SLOTS).astype(jnp.int32)
    ghost_lists = draw_ghost_lists(jax.random.fold_in(streams_of[11], 71), 0)
    star_position = jnp.clip(1.0 * jax.random.uniform(streams_of[5], (3, STARS), jnp.float32) ** levels(streams_of[5], (3, STARS), ((1, 32),), -0.2, 0.2), 0.0, 1.0)
    star_energy = jnp.clip(jnp.exp(math.log(10.0) - 4.6051702 * jax.random.uniform(streams_of[6], (STARS,), jnp.float32) ** levels(streams_of[6], (STARS,), ((0, 32),), -0.2, 0.2)), 0.1, 10.0)
    star_momentum = gaussian(streams_of[7], (3, STARS), 1.0, 6.0, ((1, 32),), jnp.float32)
    block_counts = set_ends(jax.random.randint(streams_of[8], (STAR_BLOCKS,), 1, STARS_BLOCK + 1), jax.random.fold_in(streams_of[8], 1), 1, STARS_BLOCK).astype(jnp.int32)
    block_owners_keys = jax.random.split(jax.random.fold_in(streams_of[9], 1), STAR_BLOCKS // BLOCKS)
    block_owners_turns = jax.random.permutation(jax.random.fold_in(streams_of[9], 3), STAR_BLOCKS // BLOCKS)
    block_owners = jax.vmap(lambda own, number: assign_block(jax.random.fold_in(streams_of[9], 2), own, number, BLOCKS, OWNERS, 1, SLOTS, 2))(block_owners_keys, block_owners_turns).reshape((STAR_BLOCKS, 1))
    block_leaves = set_ends(jax.random.randint(streams_of[10], (STAR_BLOCKS,), 0, LEAVES), jax.random.fold_in(streams_of[10], 1), 0, LEAVES - 1).astype(jnp.int32)
    return {"gas_position": gas_position, "gas_mass": gas_mass, "gas_smoothing": gas_smoothing, "leaf_counts": leaf_counts, "ghost_lists": ghost_lists, "star_position": star_position, "star_energy": star_energy, "star_momentum": star_momentum, "block_counts": block_counts, "block_owners": block_owners, "block_leaves": block_leaves}


SPLIT_SQ = 1.0
SOFT_SQ = 0.01
GRAVITY = 0.002
RADIAL_PUSH = 1.0

def pair_accel(targets, sources, source_mass):
    sep_x = sources[0][None, :] - targets[0][:, None]
    sep_y = sources[1][None, :] - targets[1][:, None]
    sep_z = sources[2][None, :] - targets[2][:, None]
    distance = sep_x * sep_x + sep_y * sep_y + sep_z * sep_z
    soften = distance + SOFT_SQ
    kernel = source_mass[None, :] * jnp.exp(-distance / SPLIT_SQ) / (soften * jnp.sqrt(soften))
    return GRAVITY * jnp.stack([lax.optimization_barrier(jnp.sum(sep_x * kernel, axis=1)), lax.optimization_barrier(jnp.sum(sep_y * kernel, axis=1)), lax.optimization_barrier(jnp.sum(sep_z * kernel, axis=1))])

def deposit_block(star_xyz, energy_in, momentum_in, gas_xyz, inverse):
    seps = [gas_xyz[axis_num][None, :] - star_xyz[axis_num][:, None] for axis_num in range(3)]
    distance = seps[0] * seps[0] + seps[1] * seps[1] + seps[2] * seps[2]
    weight = jnp.exp(-distance * inverse[None, :])
    normaliser = 1.0 + lax.optimization_barrier(jnp.sum(weight, axis=1))
    shares = weight / normaliser[:, None]
    heated = lax.optimization_barrier(jnp.sum(energy_in[:, None] * shares, axis=0))
    kicks = [lax.optimization_barrier(jnp.sum(shares * (momentum_in[axis_num][:, None] + RADIAL_PUSH * energy_in[:, None] * seps[axis_num]), axis=0)) for axis_num in range(3)]
    return jnp.stack([heated] + kicks)

def reference(gas_position, gas_mass, gas_smoothing, leaf_counts, ghost_lists, star_position, star_energy, star_momentum, block_counts, block_owners, block_leaves):
    grid = (N_GX, N_GY, N_GZ)
    slot_iota = jnp.arange(LEAF_SLOTS, dtype=jnp.int32)
    alive = slot_iota < leaf_counts.reshape(grid + (LEAVES, 1))
    masses = jnp.where(alive, gas_mass.reshape(grid + (LEAVES, LEAF_SLOTS)), jnp.float32(0.0))
    carried = jnp.concatenate([gas_position.reshape((3,) + grid + (LEAVES, LEAF_SLOTS)), masses[None]], axis=0)
    chosen_all = ghost_lists.reshape(grid + (4, GHOSTS))

    def select_ghosts(which):
        chosen = jnp.broadcast_to(chosen_all[None, :, :, :, which, :, None], (4,) + grid + (GHOSTS, LEAF_SLOTS))
        return jnp.take_along_axis(carried, chosen, axis=4)
    arrivals = []
    for which, shift_by, grid_axis, component, offset in ((0, 1, 1, 0, -1.0), (1, -1, 1, 0, 1.0), (2, 1, 2, 1, -1.0), (3, -1, 2, 1, 1.0)):
        moved = jnp.roll(select_ghosts(which), shift_by, axis=grid_axis)
        moved = moved.at[component].add(offset)
        arrivals.append(moved.reshape(4, DEVICES, GHOSTS * LEAF_SLOTS))
    sources = jnp.concatenate([carried.reshape(4, DEVICES, LEAVES * LEAF_SLOTS)] + arrivals, axis=2).transpose(1, 0, 2)
    targets = gas_position.reshape(3, DEVICES, LEAVES * LEAF_SLOTS).transpose(1, 0, 2)
    accel_all = lax.map(lambda pair_items: pair_accel(pair_items[0], pair_items[1][:3], pair_items[1][3]), (targets, sources))
    alive_flat = alive.reshape(PARTICLES)
    accel = jnp.where(alive_flat[None, :], accel_all.transpose(1, 0, 2).reshape(3, PARTICLES), jnp.float32(0.0))
    star_live = jnp.arange(STARS_BLOCK, dtype=jnp.int32)[None, :] < block_counts[:, None]
    star_xyz = star_position.reshape(3, STAR_BLOCKS, STARS_BLOCK).transpose(1, 0, 2)
    energy_in = jnp.where(star_live, star_energy.reshape(STAR_BLOCKS, STARS_BLOCK), jnp.float32(0.0))
    momentum_in = jnp.where(star_live[:, None, :], star_momentum.reshape(3, STAR_BLOCKS, STARS_BLOCK).transpose(1, 0, 2), jnp.float32(0.0))
    source_dev = jnp.arange(STAR_BLOCKS, dtype=jnp.int32) // BLOCKS
    dest_dev = source_dev // OWNERS * OWNERS + block_owners[:, 0].astype(jnp.int32)
    gas_leaf = (dest_dev * LEAVES + block_leaves).astype(jnp.int32)
    gas_xyz = gas_position.reshape(3, DEVICES * LEAVES, LEAF_SLOTS).transpose(1, 0, 2)
    inverse = (1.0 / (gas_smoothing * gas_smoothing)).reshape(DEVICES * LEAVES, LEAF_SLOTS)

    def one_block(items):
        xyz, energy_one, momentum_one, leaf_id = items
        return deposit_block(xyz, energy_one, momentum_one, gas_xyz[leaf_id], inverse[leaf_id])
    per_block = lax.map(one_block, (star_xyz, energy_in, momentum_in, gas_leaf), batch_size=64)
    totals = jax.ops.segment_sum(per_block, gas_leaf, num_segments=DEVICES * LEAVES)
    deposit = jnp.where(alive_flat[None, :], totals.transpose(1, 0, 2).reshape(4, PARTICLES), jnp.float32(0.0))
    return (accel, deposit)
```

```python
import functools
import math

import jax
import jax.numpy as jnp
import numpy as np
from jax import lax
from jax.experimental import pallas as pl
from jax.experimental.pallas import tpu as pltpu
from jax.sharding import PartitionSpec as P

LANES = 128
SLOTS = 3
SPLIT_SQ = 1.0
SOFT_SQ = 0.01
GRAVITY = 0.002
RADIAL_PUSH = 1.0

LOG2E = math.log2(math.e)
SCALE = LOG2E / (1.5 * SPLIT_SQ)
FACTOR = GRAVITY * math.exp(SOFT_SQ / SPLIT_SQ) * SCALE**1.5
MESH = pl.DeviceIdType.MESH
F32 = jnp.float32
BF16 = jnp.bfloat16

TILE = 256
FEATURES = 48
UNROLL = 8


def split3(x):
    a = x.astype(BF16).astype(F32)
    rest = x - a
    b = rest.astype(BF16).astype(F32)
    return a, b, rest - b


def prepare_sends(
    sizes,
    pos_ref, mass_ref, count_ref, ghost_ref,
    star_pos_ref, energy_ref, star_mom_ref, block_count_ref, owner_ref, leaf_ref,
    own, ghost_send, star_send,
):
    n_x, n_y, n_z, leaves, ghosts, blocks = sizes
    owners = n_y * n_z
    rows = leaves * LANES
    lane = lax.broadcasted_iota(jnp.int32, (1, LANES), 1)

    own[0:3, :] = pos_ref[...]
    own[4:8, :] = jnp.zeros((4, rows), F32)
    for l in range(leaves):
        here = slice(l * LANES, (l + 1) * LANES)
        alive = lane < count_ref[l]
        own[3:4, here] = jnp.where(alive, mass_ref[l : l + 1, :], 0.0)
    for k in range(4):
        for g in range(ghosts):
            leaf = ghost_ref[k * ghosts + g]
            start = pl.multiple_of(leaf * LANES, LANES)
            here = slice(g * LANES, (g + 1) * LANES)
            ghost_send[k, :, here] = own[:, pl.ds(start, LANES)]
            ghost_send[k, 7:8, here] = jnp.full((1, LANES), count_ref[leaf].astype(F32))

    @pl.loop(0, owners)
    def _(o):
        def scan(b, found):
            hit = owner_ref[b] == o
            i0, i1, i2 = found
            return (jnp.where(hit, b, i0), jnp.where(hit, i0, i1), jnp.where(hit, i1, i2))

        none = jnp.int32(-1)
        found = lax.fori_loop(0, blocks, scan, (none,) * SLOTS, unroll=8)
        for k in range(SLOTS):
            b = jnp.maximum(found[k], 0)
            valid = found[k] >= 0
            start = pl.multiple_of(b * LANES, LANES)
            count = jnp.where(valid, block_count_ref[b], 0)
            live = lane < count
            leaf = leaf_ref[b].astype(F32)
            star_send[o, k, 0:3] = star_pos_ref[:, pl.ds(start, LANES)]
            star_send[o, k, 3:4] = jnp.where(live, energy_ref[pl.ds(b, 1), :], 0.0)
            star_send[o, k, 4:7] = jnp.where(live, star_mom_ref[:, pl.ds(start, LANES)], 0.0)
            star_send[o, k, 7:8] = jnp.where(lane == 0, leaf, count.astype(F32))


def exchange(
    sizes,
    ghost_send, star_send,
    ghost_recv, star_recv, meta,
    ghost_ssem, ghost_rsem, star_ssem, star_rsem,
):
    n_x, n_y, n_z, leaves, ghosts, blocks = sizes
    owners = n_y * n_z
    x, y, z = lax.axis_index("gx"), lax.axis_index("gy"), lax.axis_index("gz")
    me = y * n_z + z

    def owner_at(d):
        other = lax.rem(me + d, owners)
        return other, (x, lax.div(other, n_z), lax.rem(other, n_z))

    def beside(k):
        step = 1 if k % 2 == 0 else -1
        if k < 2:
            return (lax.rem(x + step + n_x, n_x), y, z)
        return (x, lax.rem(y + step + n_y, n_y), z)

    barrier = pltpu.get_barrier_semaphore()
    for k in range(2):
        pl.semaphore_signal(barrier, inc=1, device_id=beside(k), device_id_type=MESH)

    @pl.loop(1, owners)
    def _(d):
        pl.semaphore_signal(barrier, inc=1, device_id=owner_at(d)[1], device_id_type=MESH)

    pl.semaphore_wait(barrier, owners + 1)

    def ghost_copy(k):
        return pltpu.make_async_remote_copy(
            src_ref=ghost_send.at[k], dst_ref=ghost_recv.at[k],
            send_sem=ghost_ssem.at[k], recv_sem=ghost_rsem.at[k],
            device_id=beside(k), device_id_type=MESH,
        )

    def star_copy(d):
        other, where = owner_at(d)
        return pltpu.make_async_remote_copy(
            src_ref=star_send.at[other], dst_ref=star_recv.at[me],
            send_sem=star_ssem.at[d], recv_sem=star_rsem.at[d],
            device_id=where, device_id_type=MESH,
        )

    @pl.loop(1, owners)
    def _(d):
        star_copy(d).start()

    for k in range(4):
        ghost_copy(k).start()
    star_recv[me] = star_send[me]
    for k in range(4):
        ghost_copy(k).wait()

    @pl.loop(1, owners)
    def _(d):
        star_copy(d).wait()

    for k in range(4):
        for g in range(ghosts):
            at = k * ghosts + g
            meta[at : at + 1, :] = ghost_recv[k, 7:8, g * LANES : (g + 1) * LANES]

    @pl.loop(0, owners)
    def _(o):
        for k in range(SLOTS):
            meta[pl.ds(4 * ghosts + o * SLOTS + k, 1), :] = star_recv[o, k, 7:8]


def gravity(
    sizes,
    count_ref, meta_ref, first_ref, second_ref,
    own_ref, smooth_ref, ghost_ref, star_ref,
    accel_ref, deposit_ref,
    comp, side_a, side_b, weights, acc, res,
    d0, d1, h0, h1, l0, l1,
    offsets, one_i, one_j, slots,
):
    n_x, n_y, n_z, leaves, ghosts, blocks = sizes
    owners = n_y * n_z
    rows = leaves * LANES
    capacity = comp.shape[1]
    trash = acc.shape[1] // TILE - 1
    lane = lax.broadcasted_iota(jnp.int32, (8, LANES), 1)
    sub = lax.broadcasted_iota(jnp.int32, (8, LANES), 0)
    wide_sub = lax.broadcasted_iota(jnp.int32, (8, TILE), 0)

    def place(tile, count, off, current):
        turn = lax.rem(off, LANES)
        base = pl.multiple_of(off - turn, LANES)
        rolled = pltpu.roll(tile, turn, 1)
        current = jnp.where(lane >= turn, rolled, current)
        comp[:, pl.ds(base, LANES)] = current
        return off + count, jnp.where(turn + count >= LANES, rolled, current)

    def own_leaf(l, carry):
        offsets[l] = carry[0]
        start = pl.multiple_of(l * LANES, LANES)
        return place(own_ref[:, pl.ds(start, LANES)], count_ref[l], *carry)

    carry = lax.fori_loop(
        0, leaves, own_leaf, (jnp.int32(0), jnp.zeros((8, LANES), F32)), unroll=8
    )
    n_own = carry[0]
    for k in range(4):
        shift = jnp.where(sub == k // 2, -1.0 if k % 2 == 0 else 1.0, 0.0)
        for g in range(ghosts):
            tile = ghost_ref[k, :, g * LANES : (g + 1) * LANES] + shift
            count = meta_ref[k * ghosts + g, 0].astype(jnp.int32)
            carry = place(tile, count, *carry)
    n_all, current = carry
    turn = lax.rem(n_all, LANES)
    base = n_all - turn
    comp[:, pl.ds(pl.multiple_of(base, LANES), LANES)] = jnp.where(lane < turn, current, 0.0)
    for extra in range(1, TILE // LANES):
        at = pl.multiple_of(base + extra * LANES, LANES)
        comp[:, pl.ds(at, LANES)] = jnp.zeros((8, LANES), F32)
    targets = lax.div(n_own + (TILE - 1), TILE)
    sources = lax.div(n_all + (TILE - 1), TILE)

    def features(parts):
        return jnp.concatenate(parts, axis=0)

    def prepare(c, _):
        here = pl.ds(pl.multiple_of(c * TILE, TILE), TILE)
        tile = comp[:, here]
        u = tile - 0.5
        mass = tile[3:4]
        norm = SCALE * (u[0:1] * u[0:1] + u[1:2] * u[1:2] + u[2:3] * u[2:3])
        one = jnp.where(wide_sub == 4, 1.0, 0.0)
        left = jnp.where(
            wide_sub < 3, (-2.0 * SCALE) * u, jnp.where(wide_sub == 3, norm + SCALE * SOFT_SQ, one)
        )
        p0, p1, p2 = split3(left)
        side_a[here, :] = features([p0, p0, p1, p1, p0, p2]).T.astype(BF16)
        one = jnp.where(wide_sub == 3, 1.0, 0.0)
        right = jnp.where(wide_sub < 3, u, jnp.where(wide_sub == 4, norm, one))
        q0, q1, q2 = split3(right)
        side_b[:, here] = features([q0, q1, q0, q1, q2, q0]).astype(BF16)
        w0, w1, w2 = split3(jnp.where(wide_sub < 3, mass * u, jnp.where(wide_sub == 3, mass, 0.0)))
        w02 = jnp.where(wide_sub < 4, w0, pltpu.roll(w2, 4, 0))
        weights[:, here] = features([w02, w1]).astype(BF16)
        acc[:, here] = jnp.zeros((16, TILE), F32)
        return 0

    lax.fori_loop(0, sources, prepare, 0)

    distance, high, low = (d0, d1), (h0, h1), (l0, l1)

    def at(block):
        return pl.ds(pl.multiple_of(block * TILE, TILE), TILE)

    def nn(a, b):
        return jnp.dot(a, b, preferred_element_type=F32)

    def nt(a, b):
        return lax.dot_general(a, b, (((1,), (1,)), ((), ())), preferred_element_type=F32)

    def tiles(table_i, table_j, count, both):
        def step(p, even):
            q = jnp.maximum(p - 2, 0)
            valid = jnp.logical_and(p >= 2, p - 2 < count)
            i, j = table_i[q], table_j[q]
            to_i = at(jnp.where(valid, i, trash))
            h, l = high[even][...], low[even][...]
            w = weights[:, at(j)]
            acc[:, to_i] = acc[:, to_i] + (nn(w, h) + nn(w, l))
            if both:
                to_j = at(jnp.where(valid, j, trash))
                w = weights[:, at(i)]
                acc[:, to_j] = acc[:, to_j] + (nt(w, h) + nt(w, l))
            d = distance[1 - even][...]
            value = jnp.exp2(-1.5 * (d + lax.log2(d)))
            h = value.astype(BF16)
            high[1 - even][...] = h
            low[1 - even][...] = (value - h.astype(F32)).astype(BF16)
            distance[even][...] = nn(side_a[at(table_j[p]), :], side_b[:, at(table_i[p])])

        @pl.loop(0, lax.div(count + 2 + UNROLL - 1, UNROLL))
        def _(g):
            for u in range(UNROLL):
                step(g * UNROLL + u, u % 2)

    def diagonal(i, n):
        one_i[n] = i
        one_j[n] = i
        return n + 1

    def column(s, n):
        def entry(i, n):
            one_i[n] = i
            one_j[n] = s
            return n + 1

        return lax.fori_loop(0, targets, entry, n)

    single = lax.fori_loop(0, targets, diagonal, jnp.int32(0))
    single = lax.fori_loop(targets, sources, column, single)
    for e in range(UNROLL + 2):
        one_i[single + e] = 0
        one_j[single + e] = 0

    tiles(first_ref, second_ref, lax.div(targets * (targets - 1), 2), True)
    tiles(one_i, one_j, single, False)

    def finish(c, _):
        here = pl.ds(pl.multiple_of(c * TILE, TILE), TILE)
        head, tail = acc[0:8, here], acc[8:16, here]
        total = head + pltpu.roll(head, 4, 0) + tail
        res[:, here] = FACTOR * (total - (comp[:, here] - 0.5) * total[3:4])
        return 0

    lax.fori_loop(0, targets, finish, 0)

    def spread(l, _):
        off = offsets[l]
        turn = lax.rem(off, LANES)
        base = pl.multiple_of(off - turn, LANES)
        both = jnp.where(
            lane >= turn,
            res[:, pl.ds(base, LANES)],
            res[:, pl.ds(pl.multiple_of(base + LANES, LANES), LANES)],
        )
        back = pltpu.roll(both, lax.rem(LANES - turn, LANES), 1)
        start = pl.multiple_of(l * LANES, LANES)
        accel_ref[:, pl.ds(start, LANES)] = jnp.where(lane < count_ref[l], back, 0.0)[0:3]
        deposit_ref[:, pl.ds(start, LANES)] = jnp.zeros((4, LANES), F32)
        return 0

    lax.fori_loop(0, leaves, spread, 0, unroll=8)

    def valid_slot(s, n):
        slots[n] = s
        return n + jnp.where(meta_ref[4 * ghosts + s, 1] > 0.5, 1, 0)

    n_slots = lax.fori_loop(0, owners * SLOTS, valid_slot, jnp.int32(0))
    group = 4
    for e in range(group):
        slots[n_slots + e] = 0

    def heat(n):
        s = slots[n]
        star = star_ref[s]
        leaf = meta_ref[4 * ghosts + s, 0].astype(jnp.int32)
        there = pl.ds(pl.multiple_of(leaf * LANES, LANES), LANES)
        gas = own_ref[:, there] - 0.5
        h = smooth_ref[pl.ds(leaf, 1), :]
        inverse = LOG2E / (h * h)
        ys = star - 0.5
        gas_norm = gas[0:1] * gas[0:1] + gas[1:2] * gas[1:2] + gas[2:3] * gas[2:3]
        star_norm = ys[0:1] * ys[0:1] + ys[1:2] * ys[1:2] + ys[2:3] * ys[2:3]
        left = jnp.where(
            sub < 3,
            (2.0 * inverse) * gas,
            jnp.where(sub == 3, -inverse * gas_norm, jnp.where(sub == 4, -inverse, 0.0)),
        )
        right = jnp.where(
            sub < 3, ys, jnp.where(sub == 3, 1.0, jnp.where(sub == 4, star_norm, 0.0))
        )
        p0, p1, p2 = split3(left)
        q0, q1, q2 = split3(right)
        a = features([p0, p0, p1, p1, p0, p2]).T.astype(BF16)
        b = features([q0, q1, q0, q1, q2, q0]).astype(BF16)
        weight = jnp.exp2(nn(a, b))
        share = 1.0 / (1.0 + jnp.sum(weight, axis=0, keepdims=True))
        energy = star[3:4]
        momentum = pltpu.roll(star, 4, 0)
        value = jnp.where(sub < 3, momentum - RADIAL_PUSH * energy * ys, energy) * share
        value = jnp.where(sub < 4, value, 0.0)
        v0, v1, v2 = split3(value)
        v02 = jnp.where(sub < 4, v0, pltpu.roll(v2, 4, 0))
        v = features([v02, v1]).astype(BF16)
        hi = weight.astype(BF16)
        lo = (weight - hi.astype(F32)).astype(BF16)
        out = nt(v, hi) + nt(v, lo)
        head, tail = out[0:8], out[8:16]
        total = head + pltpu.roll(head, 4, 0) + tail
        heat_here = total[3:4]
        kick = pltpu.roll(total + RADIAL_PUSH * heat_here * gas, 1, 0)
        both = jnp.where(sub == 0, heat_here, kick)
        live = jnp.where(n < n_slots, count_ref[leaf], 0)
        return there, jnp.where(lane < live, both, 0.0)[0:4]

    @pl.loop(0, lax.div(n_slots + group - 1, group))
    def _(t):
        done = [heat(t * group + e) for e in range(group)]
        for there, add in done:
            deposit_ref[:, there] = deposit_ref[:, there] + add


def on_device(
    mesh_sizes,
    gas_position, gas_mass, gas_smoothing, leaf_counts, ghost_lists,
    star_position, star_energy, star_momentum, block_counts, block_owners, block_leaves,
):
    n_x, n_y, n_z = mesh_sizes
    leaves = leaf_counts.shape[0]
    blocks = block_counts.shape[0]
    ghosts = ghost_lists.shape[2]
    rows = leaves * LANES
    owners = n_y * n_z
    slots = owners * SLOTS
    wide = ghosts * LANES
    vmem = pl.BlockSpec(memory_space=pltpu.VMEM)
    smem = pl.BlockSpec(memory_space=pltpu.SMEM)
    sizes = (n_x, n_y, n_z, leaves, ghosts, blocks)
    ghost_shape = jax.ShapeDtypeStruct((4, 8, wide), F32)
    star_shape = jax.ShapeDtypeStruct((owners, SLOTS, 8, LANES), F32)
    own, ghost_send, star_send = pl.pallas_call(
        functools.partial(prepare_sends, sizes),
        out_shape=(jax.ShapeDtypeStruct((8, rows), F32), ghost_shape, star_shape),
        in_specs=[vmem, vmem, smem, smem, vmem, vmem, vmem, smem, smem, smem],
        out_specs=(vmem, vmem, vmem),
    )(
        gas_position,
        gas_mass.reshape(leaves, LANES),
        leaf_counts,
        ghost_lists.reshape(-1),
        star_position,
        star_energy.reshape(blocks, LANES),
        star_momentum,
        block_counts,
        block_owners.reshape(-1),
        block_leaves,
    )
    ghost, star, meta = pl.pallas_call(
        functools.partial(exchange, sizes),
        out_shape=(
            ghost_shape,
            star_shape,
            jax.ShapeDtypeStruct((4 * ghosts + slots, LANES), F32),
        ),
        in_specs=[vmem, vmem],
        out_specs=(vmem, vmem, vmem),
        scratch_shapes=[
            pltpu.SemaphoreType.DMA((4,)),
            pltpu.SemaphoreType.DMA((4,)),
            pltpu.SemaphoreType.DMA((owners,)),
            pltpu.SemaphoreType.DMA((owners,)),
        ],
        compiler_params=pltpu.CompilerParams(collective_id=0, has_side_effects=True),
    )(ghost_send, star_send)
    top = -(-rows // TILE)
    capacity = -(-(rows + 4 * wide) // TILE) * TILE + TILE
    spare = UNROLL + 4
    pairs = [(i, j) for j in range(top + 1) for i in range(j)]
    pairs = pairs + [(0, 0)] * spare
    first = jnp.asarray(np.array([a for a, _ in pairs], np.int32))
    second = jnp.asarray(np.array([b for _, b in pairs], np.int32))
    singles = (capacity // TILE) * top + spare
    return pl.pallas_call(
        functools.partial(gravity, sizes),
        out_shape=(
            jax.ShapeDtypeStruct((3, rows), F32),
            jax.ShapeDtypeStruct((4, rows), F32),
        ),
        in_specs=[smem, smem, smem, smem, vmem, vmem, vmem, vmem],
        out_specs=(vmem, vmem),
        scratch_shapes=[
            pltpu.VMEM((8, capacity), F32),
            pltpu.VMEM((capacity, FEATURES), BF16),
            pltpu.VMEM((FEATURES, capacity), BF16),
            pltpu.VMEM((16, capacity), BF16),
            pltpu.VMEM((16, capacity + TILE), F32),
            pltpu.VMEM((8, rows + 2 * TILE), F32),
            pltpu.VMEM((TILE, TILE), F32),
            pltpu.VMEM((TILE, TILE), F32),
            pltpu.VMEM((TILE, TILE), BF16),
            pltpu.VMEM((TILE, TILE), BF16),
            pltpu.VMEM((TILE, TILE), BF16),
            pltpu.VMEM((TILE, TILE), BF16),
            pltpu.SMEM((leaves,), jnp.int32),
            pltpu.SMEM((singles,), jnp.int32),
            pltpu.SMEM((singles,), jnp.int32),
            pltpu.SMEM((slots + 4,), jnp.int32),
        ],
    )(
        leaf_counts, meta, first, second,
        own, gas_smoothing.reshape(leaves, LANES), ghost, star.reshape(slots, 8, LANES),
    )


def solution(mesh):
    split = ("gx", "gy", "gz")
    placed = (
        P(None, split), P(split), P(split), P(split), P(split, None, None),
        P(None, split), P(split), P(None, split), P(split), P(split, None), P(split),
    )
    sizes = tuple(mesh.shape[axis] for axis in split)
    return jax.shard_map(
        functools.partial(on_device, sizes),
        mesh=mesh,
        in_specs=placed,
        out_specs=(P(None, split), P(None, split)),
        check_vma=False,
    )
```

```python
import functools
import math

import jax
import jax.numpy as jnp
import numpy as np
from jax import lax
from jax.experimental import pallas as pl
from jax.experimental.pallas import tpu as pltpu
from jax.sharding import PartitionSpec as P

LANES = 128
HALF = 64
SLOTS = 3
SPLIT_SQ = 1.0
SOFT_SQ = 0.01
GRAVITY = 0.002
RADIAL_PUSH = 1.0

LOG2E = math.log2(math.e)
SCALE = LOG2E / (1.5 * SPLIT_SQ)
FACTOR = GRAVITY * math.exp(SOFT_SQ / SPLIT_SQ) * SCALE**1.5
MESH = pl.DeviceIdType.MESH
F32 = jnp.float32
BF16 = jnp.bfloat16

TILE = 256
FEATURES = 48
UNROLL = 8


def split3(x):
    a = x.astype(BF16).astype(F32)
    rest = x - a
    b = rest.astype(BF16).astype(F32)
    return a, b, rest - b


def nn(a, b):
    return jnp.dot(a, b, preferred_element_type=F32)


def nt(a, b):
    return lax.dot_general(a, b, (((1,), (1,)), ((), ())), preferred_element_type=F32)


def stack(parts):
    return jnp.concatenate(parts, axis=0)


def block_at(block):
    return pl.ds(pl.multiple_of(block * TILE, TILE), TILE)


def prepare_block(c, comp, side_a, side_b, weights, acc):
    here = block_at(c)
    sub = lax.broadcasted_iota(jnp.int32, (8, TILE), 0)
    tile = comp[:, here]
    u = tile - 0.5
    mass = tile[3:4]
    norm = SCALE * (u[0:1] * u[0:1] + u[1:2] * u[1:2] + u[2:3] * u[2:3])
    one = jnp.where(sub == 4, 1.0, 0.0)
    left = jnp.where(
        sub < 3, (-2.0 * SCALE) * u, jnp.where(sub == 3, norm + SCALE * SOFT_SQ, one)
    )
    p0, p1, p2 = split3(left)
    side_a[here, :] = stack([p0, p0, p1, p1, p0, p2]).T.astype(BF16)
    one = jnp.where(sub == 3, 1.0, 0.0)
    right = jnp.where(sub < 3, u, jnp.where(sub == 4, norm, one))
    q0, q1, q2 = split3(right)
    side_b[:, here] = stack([q0, q1, q0, q1, q2, q0]).astype(BF16)
    w0, w1, w2 = split3(jnp.where(sub < 3, mass * u, jnp.where(sub == 3, mass, 0.0)))
    w02 = jnp.where(sub < 4, w0, pltpu.roll(w2, 4, 0))
    weights[:, here] = stack([w02, w1]).astype(BF16)
    acc[:, here] = jnp.zeros((16, TILE), F32)


def distances(i, j, out, side_a, side_b):
    out[...] = nn(side_a[block_at(j), :], side_b[:, block_at(i)])


def kernel_values(d_ref, high, low):
    d = d_ref[...]
    value = jnp.exp2(-1.5 * (d + lax.log2(d)))
    h = value.astype(BF16)
    high[...] = h
    low[...] = (value - h.astype(F32)).astype(BF16)


def accumulate(i, j, to_i, to_j, high, low, weights, acc, both):
    h, l = high[...], low[...]
    w = weights[:, block_at(j)]
    acc[:, block_at(to_i)] = acc[:, block_at(to_i)] + (nn(w, h) + nn(w, l))
    if both:
        w = weights[:, block_at(i)]
        acc[:, block_at(to_j)] = acc[:, block_at(to_j)] + (nt(w, h) + nt(w, l))


def prepare_sends(
    sizes,
    pos_ref, mass_ref, count_ref, ghost_ref,
    star_pos_ref, energy_ref, star_mom_ref, block_count_ref, owner_ref, leaf_ref,
    own, ghost_send, star_send,
):
    n_x, n_y, n_z, leaves, ghosts, blocks = sizes
    owners = n_y * n_z
    rows = leaves * LANES
    lane = lax.broadcasted_iota(jnp.int32, (1, LANES), 1)

    own[0:3, :] = pos_ref[...]
    own[4:8, :] = jnp.zeros((4, rows), F32)
    for l in range(leaves):
        here = slice(l * LANES, (l + 1) * LANES)
        alive = lane < count_ref[l]
        own[3:4, here] = jnp.where(alive, mass_ref[l : l + 1, :], 0.0)
    for k in range(4):
        for g in range(ghosts):
            leaf = ghost_ref[g, k]
            start = pl.multiple_of(leaf * LANES, LANES)
            here = slice(g * LANES, (g + 1) * LANES)
            ghost_send[k, :, here] = own[:, pl.ds(start, LANES)]
            ghost_send[k, 7:8, here] = jnp.full((1, LANES), count_ref[leaf].astype(F32))

    @pl.loop(0, owners)
    def _(o):
        def scan(b, found):
            hit = owner_ref[b] == o
            i0, i1, i2 = found
            return (jnp.where(hit, b, i0), jnp.where(hit, i0, i1), jnp.where(hit, i1, i2))

        none = jnp.int32(-1)
        found = lax.fori_loop(0, blocks, scan, (none,) * SLOTS, unroll=8)
        for k in range(SLOTS):
            b = jnp.maximum(found[k], 0)
            valid = found[k] >= 0
            start = pl.multiple_of(b * LANES, LANES)
            count = jnp.where(valid, block_count_ref[b], 0)
            live = lane < count
            leaf = leaf_ref[b].astype(F32)
            star_send[o, k, 0:3] = star_pos_ref[:, pl.ds(start, LANES)]
            star_send[o, k, 3:4] = jnp.where(live, energy_ref[pl.ds(b, 1), :], 0.0)
            star_send[o, k, 4:7] = jnp.where(live, star_mom_ref[:, pl.ds(start, LANES)], 0.0)
            star_send[o, k, 7:8] = jnp.where(lane == 0, leaf, count.astype(F32))


def exchange(
    sizes,
    own, ghost_send, star_send,
    ghost_recv, star_recv, meta, comp, side_a, side_b, weights, acc,
    d0, d1, h0, h1, l0, l1,
    ghost_ssem, ghost_rsem, star_ssem, star_rsem,
):
    n_x, n_y, n_z, leaves, ghosts, blocks = sizes
    owners = n_y * n_z
    x, y, z = lax.axis_index("gx"), lax.axis_index("gy"), lax.axis_index("gz")
    me = y * n_z + z

    def owner_at(d):
        other = lax.rem(me + d, owners)
        return other, (x, lax.div(other, n_z), lax.rem(other, n_z))

    def beside(k):
        step = 1 if k % 2 == 0 else -1
        if k < 2:
            return (lax.rem(x + step + n_x, n_x), y, z)
        return (x, lax.rem(y + step + n_y, n_y), z)

    barrier = pltpu.get_barrier_semaphore()
    for k in range(2):
        pl.semaphore_signal(barrier, inc=1, device_id=beside(k), device_id_type=MESH)

    @pl.loop(1, owners)
    def _(d):
        pl.semaphore_signal(barrier, inc=1, device_id=owner_at(d)[1], device_id_type=MESH)

    lane = lax.broadcasted_iota(jnp.int32, (8, LANES), 1)
    for t in range(leaves // 2):
        left = own[:, 2 * t * LANES : (2 * t + 1) * LANES]
        right = own[:, (2 * t + 1) * LANES : (2 * t + 2) * LANES]
        comp[:, t * LANES : (t + 1) * LANES] = jnp.where(
            lane < HALF, left, pltpu.roll(right, HALF, 1)
        )

    pl.semaphore_wait(barrier, owners + 1)

    def ghost_copy(k):
        return pltpu.make_async_remote_copy(
            src_ref=ghost_send.at[k], dst_ref=ghost_recv.at[k],
            send_sem=ghost_ssem.at[k], recv_sem=ghost_rsem.at[k],
            device_id=beside(k), device_id_type=MESH,
        )

    def star_copy(d):
        other, where = owner_at(d)
        return pltpu.make_async_remote_copy(
            src_ref=star_send.at[other], dst_ref=star_recv.at[me],
            send_sem=star_ssem.at[d], recv_sem=star_rsem.at[d],
            device_id=where, device_id_type=MESH,
        )

    @pl.loop(1, owners)
    def _(d):
        star_copy(d).start()

    for k in range(4):
        ghost_copy(k).start()
    star_recv[me] = star_send[me]

    firm = comp.shape[1] // TILE

    @pl.loop(0, firm)
    def _(c):
        prepare_block(c, comp, side_a, side_b, weights, acc)

    distance, high, low = (d0, d1), (h0, h1), (l0, l1)

    def pair(p):
        i = p % firm
        return i, (i + 1 + p // firm) % firm

    count = firm * (firm - 1) // 2
    distances(*pair(0), d0, side_a, side_b)
    kernel_values(d0, h0, l0)
    distances(*pair(1), d1, side_a, side_b)
    unroll = next(u for u in (14, 10, 8, 6, 4, 2, 1) if count % u == 0)
    assert unroll % 2 == 0

    @pl.loop(0, count // unroll)
    def _(g):
        for e in range(unroll):
            p = g * unroll + e
            i, j = pair(p)
            even = e % 2
            accumulate(i, j, i, j, high[even], low[even], weights, acc, True)
            kernel_values(distance[1 - even], high[1 - even], low[1 - even])
            distances(*pair(p + 2), distance[even], side_a, side_b)

    for k in range(4):
        ghost_copy(k).wait()

    @pl.loop(1, owners)
    def _(d):
        star_copy(d).wait()

    for k in range(4):
        for g in range(ghosts):
            at = k * ghosts + g
            meta[at : at + 1, :] = ghost_recv[k, 7:8, g * LANES : (g + 1) * LANES].astype(jnp.int32)

    @pl.loop(0, owners)
    def _(o):
        for k in range(SLOTS):
            meta[pl.ds(4 * ghosts + o * SLOTS + k, 1), :] = star_recv[o, k, 7:8].astype(jnp.int32)


def gravity(
    sizes,
    count_ref, meta_ref, first_ref, second_ref,
    own_ref, smooth_ref, ghost_ref, star_ref,
    comp_in, a_in, b_in, weights_in, acc_in,
    accel_ref, deposit_ref,
    comp, side_a, side_b, weights, acc, res,
    d0, d1, h0, h1, l0, l1,
    offsets, one_i, one_j, slots, sems,
):
    n_x, n_y, n_z, leaves, ghosts, blocks = sizes
    owners = n_y * n_z
    rows = leaves * LANES
    capacity = comp.shape[1]
    trash = acc.shape[1] // TILE - 1
    lane = lax.broadcasted_iota(jnp.int32, (8, LANES), 1)
    sub = lax.broadcasted_iota(jnp.int32, (8, LANES), 0)
    settled = comp_in.shape[1]
    firm = settled // TILE

    copies = [
        pltpu.make_async_copy(comp_in, comp.at[:, 0:settled], sems.at[0]),
        pltpu.make_async_copy(a_in, side_a.at[0:settled, :], sems.at[1]),
        pltpu.make_async_copy(b_in, side_b.at[:, 0:settled], sems.at[2]),
        pltpu.make_async_copy(weights_in, weights.at[:, 0:settled], sems.at[3]),
        pltpu.make_async_copy(acc_in, acc.at[:, 0:settled], sems.at[4]),
    ]
    for copy in copies:
        copy.start()

    def place(tile, count, skip, off, current):
        turn = lax.rem(off, LANES)
        base = pl.multiple_of(off - turn, LANES)
        rolled = pltpu.roll(tile, lax.rem(turn + (LANES - skip), LANES), 1)
        current = jnp.where(lane >= turn, rolled, current)
        comp[:, pl.ds(base, LANES)] = current
        return off + count, jnp.where(turn + count >= LANES, rolled, current)

    def own_leaf(l, carry):
        offsets[l] = carry[0]
        start = pl.multiple_of(l * LANES, LANES)
        return place(own_ref[:, pl.ds(start, LANES)], count_ref[l] - HALF, HALF, *carry)

    carry = lax.fori_loop(
        0, leaves, own_leaf, (jnp.int32(settled), jnp.zeros((8, LANES), F32)), unroll=8
    )
    n_own = carry[0]
    for k in range(4):
        shift = jnp.where(sub == k // 2, -1.0 if k % 2 == 0 else 1.0, 0.0)
        for g in range(ghosts):
            tile = ghost_ref[k, :, g * LANES : (g + 1) * LANES] + shift
            count = meta_ref[k * ghosts + g, 0]
            carry = place(tile, count, 0, *carry)
    n_all, current = carry
    turn = lax.rem(n_all, LANES)
    base = n_all - turn
    comp[:, pl.ds(pl.multiple_of(base, LANES), LANES)] = jnp.where(lane < turn, current, 0.0)
    for extra in range(1, TILE // LANES):
        at = pl.multiple_of(base + extra * LANES, LANES)
        comp[:, pl.ds(at, LANES)] = jnp.zeros((8, LANES), F32)
    targets = lax.div(n_own + (TILE - 1), TILE)
    sources = lax.div(n_all + (TILE - 1), TILE)

    for copy in copies:
        copy.wait()

    def prepare(c, _):
        prepare_block(c, comp, side_a, side_b, weights, acc)
        return 0

    lax.fori_loop(firm, sources, prepare, 0)

    distance, high, low = (d0, d1), (h0, h1), (l0, l1)

    def tiles(table_i, table_j, begin, count, both):
        def step(p, even):
            q = jnp.maximum(p - 2, begin)
            valid = jnp.logical_and(p >= begin + 2, p - 2 < count)
            i, j = table_i[q], table_j[q]
            to_i, to_j = jnp.where(valid, i, trash), jnp.where(valid, j, trash)
            accumulate(i, j, to_i, to_j, high[even], low[even], weights, acc, both)
            kernel_values(distance[1 - even], high[1 - even], low[1 - even])
            distances(table_i[p], table_j[p], distance[even], side_a, side_b)

        @pl.loop(0, lax.div(count - begin + 2 + UNROLL - 1, UNROLL))
        def _(g):
            for u in range(UNROLL):
                step(begin + g * UNROLL + u, u % 2)

    def diagonal(i, n):
        one_i[n] = i
        one_j[n] = i
        return n + 1

    def column(s, n):
        def entry(i, n):
            one_i[n] = i
            one_j[n] = s
            return n + 1

        return lax.fori_loop(0, targets, entry, n)

    single = lax.fori_loop(0, targets, diagonal, jnp.int32(0))
    single = lax.fori_loop(targets, sources, column, single)
    for e in range(UNROLL + 2):
        one_i[single + e] = 0
        one_j[single + e] = 0

    done = firm * (firm - 1) // 2
    tiles(first_ref, second_ref, done, lax.div(targets * (targets - 1), 2), True)
    tiles(one_i, one_j, 0, single, False)

    def finish(c, _):
        here = block_at(c)
        head, tail = acc[0:8, here], acc[8:16, here]
        total = head + pltpu.roll(head, 4, 0) + tail
        res[:, here] = FACTOR * (total - (comp[:, here] - 0.5) * total[3:4])
        return 0

    lax.fori_loop(0, targets, finish, 0)

    def spread(l, side):
        off = offsets[l]
        turn = lax.rem(off, LANES)
        base = pl.multiple_of(off - turn, LANES)
        both = jnp.where(
            lane >= turn,
            res[:, pl.ds(base, LANES)],
            res[:, pl.ds(pl.multiple_of(base + LANES, LANES), LANES)],
        )
        back = pltpu.roll(both, lax.rem(LANES + HALF - turn, LANES), 1)
        back = jnp.where(lane < HALF, side, back)
        start = pl.multiple_of(l * LANES, LANES)
        accel_ref[:, pl.ds(start, LANES)] = jnp.where(lane < count_ref[l], back, 0.0)[0:3]
        deposit_ref[:, pl.ds(start, LANES)] = jnp.zeros((4, LANES), F32)

    def spread_two(t, _):
        side = res[:, pl.ds(pl.multiple_of(t * LANES, LANES), LANES)]
        spread(2 * t, side)
        spread(2 * t + 1, pltpu.roll(side, HALF, 1))
        return 0

    lax.fori_loop(0, leaves // 2, spread_two, 0, unroll=4)

    def valid_slot(s, n):
        slots[n] = s
        return n + jnp.where(meta_ref[4 * ghosts + s, 1] > 0, 1, 0)

    n_slots = lax.fori_loop(0, owners * SLOTS, valid_slot, jnp.int32(0))
    group = 4
    for e in range(group):
        slots[n_slots + e] = 0

    def heat(n):
        s = slots[n]
        star = star_ref[s]
        leaf = meta_ref[4 * ghosts + s, 0]
        there = pl.ds(pl.multiple_of(leaf * LANES, LANES), LANES)
        gas = own_ref[:, there] - 0.5
        h = smooth_ref[pl.ds(leaf, 1), :]
        inverse = LOG2E / (h * h)
        ys = star - 0.5
        gas_norm = gas[0:1] * gas[0:1] + gas[1:2] * gas[1:2] + gas[2:3] * gas[2:3]
        star_norm = ys[0:1] * ys[0:1] + ys[1:2] * ys[1:2] + ys[2:3] * ys[2:3]
        left = jnp.where(
            sub < 3,
            (2.0 * inverse) * gas,
            jnp.where(sub == 3, -inverse * gas_norm, jnp.where(sub == 4, -inverse, 0.0)),
        )
        right = jnp.where(
            sub < 3, ys, jnp.where(sub == 3, 1.0, jnp.where(sub == 4, star_norm, 0.0))
        )
        p0, p1, p2 = split3(left)
        q0, q1, q2 = split3(right)
        a = stack([p0, p0, p1, p1, p0, p2]).T.astype(BF16)
        b = stack([q0, q1, q0, q1, q2, q0]).astype(BF16)
        weight = jnp.exp2(nn(a, b))
        share = 1.0 / (1.0 + jnp.sum(weight, axis=0, keepdims=True))
        energy = star[3:4]
        momentum = pltpu.roll(star, 4, 0)
        value = jnp.where(sub < 3, momentum - RADIAL_PUSH * energy * ys, energy) * share
        value = jnp.where(sub < 4, value, 0.0)
        v0, v1, v2 = split3(value)
        v02 = jnp.where(sub < 4, v0, pltpu.roll(v2, 4, 0))
        v = stack([v02, v1]).astype(BF16)
        hi = weight.astype(BF16)
        lo = (weight - hi.astype(F32)).astype(BF16)
        out = nt(v, hi) + nt(v, lo)
        head, tail = out[0:8], out[8:16]
        total = head + pltpu.roll(head, 4, 0) + tail
        heat_here = total[3:4]
        kick = pltpu.roll(total + RADIAL_PUSH * heat_here * gas, 1, 0)
        both = jnp.where(sub == 0, heat_here, kick)
        live = jnp.where(n < n_slots, count_ref[leaf], 0)
        return there, jnp.where(lane < live, both, 0.0)[0:4]

    @pl.loop(0, lax.div(n_slots + group - 1, group))
    def _(t):
        done = [heat(t * group + e) for e in range(group)]
        for there, add in done:
            deposit_ref[:, there] = deposit_ref[:, there] + add


def on_device(
    mesh_sizes,
    gas_position, gas_mass, gas_smoothing, leaf_counts, ghost_lists,
    star_position, star_energy, star_momentum, block_counts, block_owners, block_leaves,
):
    n_x, n_y, n_z = mesh_sizes
    leaves = leaf_counts.shape[0]
    blocks = block_counts.shape[0]
    ghosts = ghost_lists.shape[2]
    rows = leaves * LANES
    owners = n_y * n_z
    slots = owners * SLOTS
    wide = ghosts * LANES
    vmem = pl.BlockSpec(memory_space=pltpu.VMEM)
    smem = pl.BlockSpec(memory_space=pltpu.SMEM)
    sizes = (n_x, n_y, n_z, leaves, ghosts, blocks)
    ghost_shape = jax.ShapeDtypeStruct((4, 8, wide), F32)
    star_shape = jax.ShapeDtypeStruct((owners, SLOTS, 8, LANES), F32)
    own, ghost_send, star_send = pl.pallas_call(
        functools.partial(prepare_sends, sizes),
        out_shape=(jax.ShapeDtypeStruct((8, rows), F32), ghost_shape, star_shape),
        in_specs=[vmem, vmem, smem, smem, vmem, vmem, vmem, smem, smem, smem],
        out_specs=(vmem, vmem, vmem),
    )(
        gas_position,
        gas_mass.reshape(leaves, LANES),
        leaf_counts,
        ghost_lists[0].T,
        star_position,
        star_energy.reshape(blocks, LANES),
        star_momentum,
        block_counts,
        block_owners.reshape(-1),
        block_leaves,
    )
    settled = leaves * HALF
    square = [pltpu.VMEM((TILE, TILE), F32)] * 2 + [pltpu.VMEM((TILE, TILE), BF16)] * 4
    ghost, star, meta, *early = pl.pallas_call(
        functools.partial(exchange, sizes),
        out_shape=(
            ghost_shape,
            star_shape,
            jax.ShapeDtypeStruct((4 * ghosts + slots, LANES), jnp.int32),
            jax.ShapeDtypeStruct((8, settled), F32),
            jax.ShapeDtypeStruct((settled, FEATURES), BF16),
            jax.ShapeDtypeStruct((FEATURES, settled), BF16),
            jax.ShapeDtypeStruct((16, settled), BF16),
            jax.ShapeDtypeStruct((16, settled), F32),
        ),
        in_specs=[vmem] * 3,
        out_specs=(vmem,) * 8,
        scratch_shapes=square + [
            pltpu.SemaphoreType.DMA((4,)),
            pltpu.SemaphoreType.DMA((4,)),
            pltpu.SemaphoreType.DMA((owners,)),
            pltpu.SemaphoreType.DMA((owners,)),
        ],
        compiler_params=pltpu.CompilerParams(collective_id=0, has_side_effects=True),
    )(own, ghost_send, star_send)
    top = -(-rows // TILE)
    capacity = -(-(rows + 4 * wide) // TILE) * TILE + TILE
    spare = UNROLL + 4
    pairs = [(i, j) for j in range(top + 1) for i in range(j)]
    pairs = pairs + [(0, 0)] * spare
    first = jnp.asarray(np.array([a for a, _ in pairs], np.int32))
    second = jnp.asarray(np.array([b for _, b in pairs], np.int32))
    singles = (capacity // TILE) * top + spare
    return pl.pallas_call(
        functools.partial(gravity, sizes),
        out_shape=(
            jax.ShapeDtypeStruct((3, rows), F32),
            jax.ShapeDtypeStruct((4, rows), F32),
        ),
        in_specs=[smem] * 4 + [vmem] * 4 + [pl.BlockSpec(memory_space=pltpu.HBM)] * 5,
        out_specs=(vmem, vmem),
        scratch_shapes=[
            pltpu.VMEM((8, capacity), F32),
            pltpu.VMEM((capacity, FEATURES), BF16),
            pltpu.VMEM((FEATURES, capacity), BF16),
            pltpu.VMEM((16, capacity), BF16),
            pltpu.VMEM((16, capacity + TILE), F32),
            pltpu.VMEM((8, rows + 2 * TILE), F32),
            *square,
            pltpu.SMEM((leaves,), jnp.int32),
            pltpu.SMEM((singles,), jnp.int32),
            pltpu.SMEM((singles,), jnp.int32),
            pltpu.SMEM((slots + 4,), jnp.int32),
            pltpu.SemaphoreType.DMA((5,)),
        ],
    )(
        leaf_counts, meta, first, second,
        own, gas_smoothing.reshape(leaves, LANES), ghost, star.reshape(slots, 8, LANES),
        *early,
    )


def solution(mesh):
    split = ("gx", "gy", "gz")
    placed = (
        P(None, split), P(split), P(split), P(split), P(split, None, None),
        P(None, split), P(split), P(None, split), P(split), P(split, None), P(split),
    )
    sizes = tuple(mesh.shape[axis] for axis in split)
    return jax.shard_map(
        functools.partial(on_device, sizes),
        mesh=mesh,
        in_specs=placed,
        out_specs=(P(None, split), P(None, split)),
        check_vma=False,
    )
```

```python
import functools
import math

import jax
import jax.numpy as jnp
import numpy as np
from jax import lax
from jax.experimental import pallas as pl
from jax.experimental.pallas import tpu as pltpu
from jax.sharding import PartitionSpec as P

LANES = 128
HALF = 64
SLOTS = 3
SPLIT_SQ = 1.0
SOFT_SQ = 0.01
GRAVITY = 0.002
RADIAL_PUSH = 1.0

LOG2E = math.log2(math.e)
SCALE = LOG2E / (1.5 * SPLIT_SQ)
FACTOR = GRAVITY * math.exp(SOFT_SQ / SPLIT_SQ) * SCALE**1.5
MESH = pl.DeviceIdType.MESH
F32 = jnp.float32
BF16 = jnp.bfloat16

TILE = 256
FEATURES = 48
UNROLL = 8
GROUP = 8


def split3(x):
    a = x.astype(BF16).astype(F32)
    rest = x - a
    b = rest.astype(BF16).astype(F32)
    return a, b, rest - b


def nn(a, b):
    return jnp.dot(a, b, preferred_element_type=F32)


def nt(a, b):
    return lax.dot_general(a, b, (((1,), (1,)), ((), ())), preferred_element_type=F32)


def stack(parts):
    return jnp.concatenate(parts, axis=0)


def block_at(block):
    return pl.ds(pl.multiple_of(block * TILE, TILE), TILE)


def prepare_block(c, comp, side_a, side_b, weights, acc):
    here = block_at(c)
    sub = lax.broadcasted_iota(jnp.int32, (8, TILE), 0)
    tile = comp[:, here]
    u = tile - 0.5
    mass = tile[3:4]
    norm = SCALE * (u[0:1] * u[0:1] + u[1:2] * u[1:2] + u[2:3] * u[2:3])
    one = jnp.where(sub == 4, 1.0, 0.0)
    left = jnp.where(
        sub < 3, (-2.0 * SCALE) * u, jnp.where(sub == 3, norm + SCALE * SOFT_SQ, one)
    )
    p0, p1, p2 = split3(left)
    side_a[here, :] = stack([p0, p0, p1, p1, p0, p2]).T.astype(BF16)
    one = jnp.where(sub == 3, 1.0, 0.0)
    right = jnp.where(sub < 3, u, jnp.where(sub == 4, norm, one))
    q0, q1, q2 = split3(right)
    side_b[:, here] = stack([q0, q1, q0, q1, q2, q0]).astype(BF16)
    w0, w1, w2 = split3(jnp.where(sub < 3, mass * u, jnp.where(sub == 3, mass, 0.0)))
    w02 = jnp.where(sub < 4, w0, pltpu.roll(w2, 4, 0))
    weights[:, here] = stack([w02, w1]).astype(BF16)
    acc[:, here] = jnp.zeros((16, TILE), F32)


def distances(i, j, out, side_a, side_b):
    out[...] = nn(side_a[block_at(j), :], side_b[:, block_at(i)])


def kernel_values(d_ref, high, low):
    d = d_ref[...]
    value = jnp.exp2(-1.5 * (d + lax.log2(d)))
    h = value.astype(BF16)
    high[...] = h
    low[...] = (value - h.astype(F32)).astype(BF16)


def accumulate(i, j, to_i, to_j, high, low, weights, acc, both):
    h, l = high[...], low[...]
    w = weights[:, block_at(j)]
    acc[:, block_at(to_i)] = acc[:, block_at(to_i)] + (nn(w, h) + nn(w, l))
    if both:
        w = weights[:, block_at(i)]
        acc[:, block_at(to_j)] = acc[:, block_at(to_j)] + (nt(w, h) + nt(w, l))


def prepare_sends(
    sizes,
    pos_ref, mass_ref, count_ref, ghost_ref,
    star_pos_ref, energy_ref, star_mom_ref, block_count_ref, owner_ref, leaf_ref,
    own, ghost_send, star_send,
):
    n_x, n_y, n_z, leaves, ghosts, blocks = sizes
    owners = n_y * n_z
    rows = leaves * LANES
    lane = lax.broadcasted_iota(jnp.int32, (1, LANES), 1)

    own[0:3, :] = pos_ref[...]
    own[4:8, :] = jnp.zeros((4, rows), F32)
    for l in range(leaves):
        here = slice(l * LANES, (l + 1) * LANES)
        alive = lane < count_ref[l]
        own[3:4, here] = jnp.where(alive, mass_ref[l : l + 1, :], 0.0)
    for k in range(4):
        for g in range(ghosts):
            leaf = ghost_ref[g, k]
            start = pl.multiple_of(leaf * LANES, LANES)
            here = slice(g * LANES, (g + 1) * LANES)
            ghost_send[k, :, here] = own[:, pl.ds(start, LANES)]
            ghost_send[k, 7:8, here] = jnp.full((1, LANES), count_ref[leaf].astype(F32))

    @pl.loop(0, owners)
    def _(o):
        def scan(b, found):
            hit = owner_ref[b] == o
            i0, i1, i2 = found
            return (jnp.where(hit, b, i0), jnp.where(hit, i0, i1), jnp.where(hit, i1, i2))

        none = jnp.int32(-1)
        found = lax.fori_loop(0, blocks, scan, (none,) * SLOTS, unroll=8)
        for k in range(SLOTS):
            b = jnp.maximum(found[k], 0)
            valid = found[k] >= 0
            start = pl.multiple_of(b * LANES, LANES)
            count = jnp.where(valid, block_count_ref[b], 0)
            live = lane < count
            leaf = leaf_ref[b].astype(F32)
            star_send[o, k, 0:3] = star_pos_ref[:, pl.ds(start, LANES)]
            star_send[o, k, 3:4] = jnp.where(live, energy_ref[pl.ds(b, 1), :], 0.0)
            star_send[o, k, 4:7] = jnp.where(live, star_mom_ref[:, pl.ds(start, LANES)], 0.0)
            star_send[o, k, 7:8] = jnp.where(lane == 0, leaf, count.astype(F32))


def exchange(
    sizes,
    own, ghost_send, star_send,
    ghost_recv, star_recv, meta, comp, side_a, side_b, weights, acc,
    d0, d1, h0, h1, l0, l1,
    ghost_ssem, ghost_rsem, star_ssem, star_rsem,
):
    n_x, n_y, n_z, leaves, ghosts, blocks = sizes
    owners = n_y * n_z
    x, y, z = lax.axis_index("gx"), lax.axis_index("gy"), lax.axis_index("gz")
    me = y * n_z + z

    def owner_at(d):
        other = lax.rem(me + d, owners)
        return other, (x, lax.div(other, n_z), lax.rem(other, n_z))

    def beside(k):
        step = 1 if k % 2 == 0 else -1
        if k < 2:
            return (lax.rem(x + step + n_x, n_x), y, z)
        return (x, lax.rem(y + step + n_y, n_y), z)

    barrier = pltpu.get_barrier_semaphore()
    for k in range(2):
        pl.semaphore_signal(barrier, inc=1, device_id=beside(k), device_id_type=MESH)

    @pl.loop(1, owners)
    def _(d):
        pl.semaphore_signal(barrier, inc=1, device_id=owner_at(d)[1], device_id_type=MESH)

    lane = lax.broadcasted_iota(jnp.int32, (8, LANES), 1)
    for t in range(leaves // 2):
        left = own[:, 2 * t * LANES : (2 * t + 1) * LANES]
        right = own[:, (2 * t + 1) * LANES : (2 * t + 2) * LANES]
        comp[:, t * LANES : (t + 1) * LANES] = jnp.where(
            lane < HALF, left, pltpu.roll(right, HALF, 1)
        )

    pl.semaphore_wait(barrier, owners + 1)

    def ghost_copy(k):
        return pltpu.make_async_remote_copy(
            src_ref=ghost_send.at[k], dst_ref=ghost_recv.at[k],
            send_sem=ghost_ssem.at[k], recv_sem=ghost_rsem.at[k],
            device_id=beside(k), device_id_type=MESH,
        )

    def star_copy(d):
        other, where = owner_at(d)
        return pltpu.make_async_remote_copy(
            src_ref=star_send.at[other], dst_ref=star_recv.at[me],
            send_sem=star_ssem.at[d], recv_sem=star_rsem.at[d],
            device_id=where, device_id_type=MESH,
        )

    @pl.loop(1, owners)
    def _(d):
        star_copy(d).start()

    for k in range(4):
        ghost_copy(k).start()
    star_recv[me] = star_send[me]

    firm = comp.shape[1] // TILE

    @pl.loop(0, firm)
    def _(c):
        prepare_block(c, comp, side_a, side_b, weights, acc)

    distance, high, low = (d0, d1), (h0, h1), (l0, l1)

    period = firm + 1
    unroll = 2 * period
    assert firm % 4 == 0

    def task(g, e):
        g, e = g + e // unroll, e % unroll
        half, r = divmod(e, period)
        middle = (firm - 1) // 2
        if r in (middle, firm):
            i = (4 * g + 2 * half + r // firm) % firm
            return i, i, False
        p = (2 * g + half) * (firm - 1) + r - r // (middle + 1)
        i = p % firm
        return i, (i + 1 + p // firm) % firm, True

    distances(*task(0, 0)[:2], d0, side_a, side_b)
    distances(*task(0, 1)[:2], d1, side_a, side_b)
    kernel_values(d0, h0, l0)

    @pl.loop(0, firm // 4)
    def _(g):
        for e in range(unroll):
            even = e % 2
            i, j, both = task(g, e)
            distances(*task(g, e + 2)[:2], distance[even], side_a, side_b)
            kernel_values(distance[1 - even], high[1 - even], low[1 - even])
            accumulate(i, j, i, j, high[even], low[even], weights, acc, both)

    for k in range(4):
        ghost_copy(k).wait()

    @pl.loop(1, owners)
    def _(d):
        star_copy(d).wait()

    for k in range(4):
        for g in range(ghosts):
            at = k * ghosts + g
            meta[at : at + 1, :] = ghost_recv[k, 7:8, g * LANES : (g + 1) * LANES].astype(jnp.int32)

    @pl.loop(0, owners)
    def _(o):
        for k in range(SLOTS):
            meta[pl.ds(4 * ghosts + o * SLOTS + k, 1), :] = star_recv[o, k, 7:8].astype(jnp.int32)


def gravity(
    sizes,
    count_ref, meta_ref, first_ref, second_ref,
    own_ref, smooth_ref, ghost_ref, star_ref,
    comp_in, a_in, b_in, weights_in, acc_in,
    accel_ref, deposit_ref,
    comp, side_a, side_b, weights, acc, res,
    d0, d1, h0, h1, l0, l1,
    star_a, star_b, star_d, star_h, star_l, star_v,
    offsets, one_i, one_j, slots, sems,
):
    n_x, n_y, n_z, leaves, ghosts, blocks = sizes
    owners = n_y * n_z
    rows = leaves * LANES
    capacity = comp.shape[1]
    trash = acc.shape[1] // TILE - 1
    lane = lax.broadcasted_iota(jnp.int32, (8, LANES), 1)
    sub = lax.broadcasted_iota(jnp.int32, (8, LANES), 0)
    settled = comp_in.shape[1]
    firm = settled // TILE

    copies = [
        pltpu.make_async_copy(comp_in, comp.at[:, 0:settled], sems.at[0]),
        pltpu.make_async_copy(a_in, side_a.at[0:settled, :], sems.at[1]),
        pltpu.make_async_copy(b_in, side_b.at[:, 0:settled], sems.at[2]),
        pltpu.make_async_copy(weights_in, weights.at[:, 0:settled], sems.at[3]),
        pltpu.make_async_copy(acc_in, acc.at[:, 0:settled], sems.at[4]),
    ]
    for copy in copies:
        copy.start()

    def place(tile, count, skip, off, current):
        turn = lax.rem(off, LANES)
        base = pl.multiple_of(off - turn, LANES)
        rolled = pltpu.roll(tile, lax.rem(turn + (LANES - skip), LANES), 1)
        current = jnp.where(lane >= turn, rolled, current)
        comp[:, pl.ds(base, LANES)] = current
        return off + count, jnp.where(turn + count >= LANES, rolled, current)

    def own_leaf(l, carry):
        offsets[l] = carry[0]
        start = pl.multiple_of(l * LANES, LANES)
        return place(own_ref[:, pl.ds(start, LANES)], count_ref[l] - HALF, HALF, *carry)

    carry = lax.fori_loop(
        0, leaves, own_leaf, (jnp.int32(settled), jnp.zeros((8, LANES), F32)), unroll=8
    )
    n_own = carry[0]
    for k in range(4):
        shift = jnp.where(sub == k // 2, -1.0 if k % 2 == 0 else 1.0, 0.0)
        for g in range(ghosts):
            tile = ghost_ref[k, :, g * LANES : (g + 1) * LANES] + shift
            count = meta_ref[k * ghosts + g, 0]
            carry = place(tile, count, 0, *carry)
    n_all, current = carry
    turn = lax.rem(n_all, LANES)
    base = n_all - turn
    comp[:, pl.ds(pl.multiple_of(base, LANES), LANES)] = jnp.where(lane < turn, current, 0.0)
    for extra in range(1, TILE // LANES):
        at = pl.multiple_of(base + extra * LANES, LANES)
        comp[:, pl.ds(at, LANES)] = jnp.zeros((8, LANES), F32)
    targets = lax.div(n_own + (TILE - 1), TILE)
    sources = lax.div(n_all + (TILE - 1), TILE)

    for copy in copies:
        copy.wait()

    def prepare(c, _):
        prepare_block(c, comp, side_a, side_b, weights, acc)
        return 0

    lax.fori_loop(firm, sources, prepare, 0)

    distance, high, low = (d0, d1), (h0, h1), (l0, l1)

    def tiles(tables, unroll):
        kinds = len(tables)
        steps = 0
        for table_i, table_j, begin, count, both in tables:
            steps = jnp.maximum(steps, kinds * (count - begin) + 2)

        def entry(u, base, ahead):
            table_i, table_j, begin, count, both = tables[(u + ahead) % kinds]
            k = begin + base + (u + ahead) // kinds
            return table_i, table_j, begin, count, both, k

        def step(base, u):
            even = u % 2
            table_i, table_j, *_, k = entry(u, base, 0)
            distances(table_i[k], table_j[k], distance[even], side_a, side_b)
            kernel_values(distance[1 - even], high[1 - even], low[1 - even])
            table_i, table_j, begin, count, both, k = entry(u, base, -2)
            valid = jnp.logical_and(k >= begin, k < count)
            q = jnp.maximum(k, begin)
            i, j = table_i[q], table_j[q]
            to_i, to_j = jnp.where(valid, i, trash), jnp.where(valid, j, trash)
            accumulate(i, j, to_i, to_j, high[even], low[even], weights, acc, both)

        @pl.loop(0, lax.div(steps + (unroll - 1), unroll))
        def _(g):
            for u in range(unroll):
                step(g * (unroll // kinds), u)

    def single(i, j, n):
        one_i[n] = i
        one_j[n] = j
        return n + 1

    def column(s, n):
        return lax.fori_loop(0, targets, lambda i, n: single(i, s, n), n)

    done = firm * (firm - 1) // 2
    n_both = lax.div(targets * (targets - 1), 2) - done
    n_one = lax.fori_loop(firm, targets, lambda i, n: single(i, i, n), jnp.int32(0))
    n_one = lax.fori_loop(targets, sources, column, n_one)

    def blank(n, _):
        one_i[n] = 0
        one_j[n] = 0
        return 0

    lax.fori_loop(n_one, jnp.maximum(n_one, n_both) + UNROLL + 2, blank, 0)
    tiles(
        [
            (first_ref, second_ref, done, done + n_both, True),
            (one_i, one_j, 0, jnp.minimum(n_one, n_both), False),
        ],
        UNROLL,
    )

    @pl.when(n_one > n_both)
    def _():
        tiles([(one_i, one_j, n_both, n_one, False)], UNROLL // 2)

    def finish(c, _):
        here = block_at(c)
        head, tail = acc[0:8, here], acc[8:16, here]
        total = head + pltpu.roll(head, 4, 0) + tail
        res[:, here] = FACTOR * (total - (comp[:, here] - 0.5) * total[3:4])
        return 0

    lax.fori_loop(0, targets, finish, 0)

    def spread(l, side):
        off = offsets[l]
        turn = lax.rem(off, LANES)
        base = pl.multiple_of(off - turn, LANES)
        both = jnp.where(
            lane >= turn,
            res[:, pl.ds(base, LANES)],
            res[:, pl.ds(pl.multiple_of(base + LANES, LANES), LANES)],
        )
        back = pltpu.roll(both, lax.rem(LANES + HALF - turn, LANES), 1)
        back = jnp.where(lane < HALF, side, back)
        start = pl.multiple_of(l * LANES, LANES)
        accel_ref[:, pl.ds(start, LANES)] = jnp.where(lane < count_ref[l], back, 0.0)[0:3]
        deposit_ref[:, pl.ds(start, LANES)] = jnp.zeros((4, LANES), F32)

    def spread_two(t, _):
        side = res[:, pl.ds(pl.multiple_of(t * LANES, LANES), LANES)]
        spread(2 * t, side)
        spread(2 * t + 1, pltpu.roll(side, HALF, 1))
        return 0

    lax.fori_loop(0, leaves // 2, spread_two, 0, unroll=4)

    def valid_slot(s, n):
        slots[n] = s
        return n + jnp.where(meta_ref[4 * ghosts + s, 1] > 0, 1, 0)

    n_slots = lax.fori_loop(0, owners * SLOTS, valid_slot, jnp.int32(0))
    def empty_slot(e, _):
        slots[e] = 0
        return 0

    lax.fori_loop(n_slots, n_slots + GROUP + 3, empty_slot, 0)

    def slot_at(n):
        s = slots[n]
        leaf = meta_ref[4 * ghosts + s, 0]
        there = pl.ds(pl.multiple_of(leaf * LANES, LANES), LANES)
        return star_ref[s], own_ref[:, there] - 0.5, leaf, there

    def star_features(n, left_out, right_out):
        star, gas, leaf, _ = slot_at(n)
        h = smooth_ref[pl.ds(leaf, 1), :]
        inverse = LOG2E / (h * h)
        ys = star - 0.5
        gas_norm = gas[0:1] * gas[0:1] + gas[1:2] * gas[1:2] + gas[2:3] * gas[2:3]
        star_norm = ys[0:1] * ys[0:1] + ys[1:2] * ys[1:2] + ys[2:3] * ys[2:3]
        left = jnp.where(
            sub < 3,
            (2.0 * inverse) * gas,
            jnp.where(sub == 3, -inverse * gas_norm, jnp.where(sub == 4, -inverse, 0.0)),
        )
        right = jnp.where(
            sub < 3, ys, jnp.where(sub == 3, 1.0, jnp.where(sub == 4, star_norm, 0.0))
        )
        p0, p1, p2 = split3(left)
        q0, q1, q2 = split3(right)
        left_out[...] = stack([p0, p0, p1, p1, p0, p2]).T.astype(BF16)
        right_out[...] = stack([q0, q1, q0, q1, q2, q0]).astype(BF16)

    def star_weights(n, exponent, high, low, value_out):
        weight = jnp.exp2(exponent[...])
        hi = weight.astype(BF16)
        high[...] = hi
        low[...] = (weight - hi.astype(F32)).astype(BF16)
        share = 1.0 / (1.0 + jnp.sum(weight, axis=0, keepdims=True))
        star = star_ref[slots[n]]
        energy = star[3:4]
        momentum = pltpu.roll(star, 4, 0)
        value = jnp.where(sub < 3, momentum - RADIAL_PUSH * energy * (star - 0.5), energy)
        v0, v1, v2 = split3(jnp.where(sub < 4, value * share, 0.0))
        v02 = jnp.where(sub < 4, v0, pltpu.roll(v2, 4, 0))
        value_out[...] = stack([v02, v1]).astype(BF16)

    def star_deposit(n, high, low, value):
        _, gas, leaf, there = slot_at(jnp.maximum(n, 0))
        v = value[...]
        out = nt(v, high[...]) + nt(v, low[...])
        head, tail = out[0:8], out[8:16]
        total = head + pltpu.roll(head, 4, 0) + tail
        heat_here = total[3:4]
        kick = pltpu.roll(total + RADIAL_PUSH * heat_here * gas, 1, 0)
        both = jnp.where(sub == 0, heat_here, kick)
        valid = jnp.logical_and(n >= 0, n < n_slots)
        live = jnp.where(valid, count_ref[leaf], 0)
        deposit_ref[:, there] = deposit_ref[:, there] + jnp.where(lane < live, both, 0.0)[0:4]

    @pl.loop(0, lax.div(n_slots + 3 + GROUP - 1, GROUP))
    def _(t):
        for e in range(GROUP):
            n, even = t * GROUP + e, e % 2
            star_features(n, star_a.at[even], star_b.at[even])
            star_d[even] = nn(star_a[1 - even], star_b[1 - even])
            star_weights(
                jnp.maximum(n - 2, 0), star_d.at[1 - even],
                star_h.at[1 - even], star_l.at[1 - even], star_v.at[1 - even],
            )
            star_deposit(n - 3, star_h.at[even], star_l.at[even], star_v.at[even])


def on_device(
    mesh_sizes,
    gas_position, gas_mass, gas_smoothing, leaf_counts, ghost_lists,
    star_position, star_energy, star_momentum, block_counts, block_owners, block_leaves,
):
    n_x, n_y, n_z = mesh_sizes
    leaves = leaf_counts.shape[0]
    blocks = block_counts.shape[0]
    ghosts = ghost_lists.shape[2]
    rows = leaves * LANES
    owners = n_y * n_z
    slots = owners * SLOTS
    wide = ghosts * LANES
    vmem = pl.BlockSpec(memory_space=pltpu.VMEM)
    smem = pl.BlockSpec(memory_space=pltpu.SMEM)
    sizes = (n_x, n_y, n_z, leaves, ghosts, blocks)
    ghost_shape = jax.ShapeDtypeStruct((4, 8, wide), F32)
    star_shape = jax.ShapeDtypeStruct((owners, SLOTS, 8, LANES), F32)
    own, ghost_send, star_send = pl.pallas_call(
        functools.partial(prepare_sends, sizes),
        out_shape=(jax.ShapeDtypeStruct((8, rows), F32), ghost_shape, star_shape),
        in_specs=[vmem, vmem, smem, smem, vmem, vmem, vmem, smem, smem, smem],
        out_specs=(vmem, vmem, vmem),
    )(
        gas_position,
        gas_mass.reshape(leaves, LANES),
        leaf_counts,
        ghost_lists[0].T,
        star_position,
        star_energy.reshape(blocks, LANES),
        star_momentum,
        block_counts,
        block_owners.reshape(-1),
        block_leaves,
    )
    settled = leaves * HALF
    square = [pltpu.VMEM((TILE, TILE), F32)] * 2 + [pltpu.VMEM((TILE, TILE), BF16)] * 4
    ghost, star, meta, *early = pl.pallas_call(
        functools.partial(exchange, sizes),
        out_shape=(
            ghost_shape,
            star_shape,
            jax.ShapeDtypeStruct((4 * ghosts + slots, LANES), jnp.int32),
            jax.ShapeDtypeStruct((8, settled), F32),
            jax.ShapeDtypeStruct((settled, FEATURES), BF16),
            jax.ShapeDtypeStruct((FEATURES, settled), BF16),
            jax.ShapeDtypeStruct((16, settled), BF16),
            jax.ShapeDtypeStruct((16, settled), F32),
        ),
        in_specs=[vmem] * 3,
        out_specs=(vmem,) * 8,
        scratch_shapes=square + [
            pltpu.SemaphoreType.DMA((4,)),
            pltpu.SemaphoreType.DMA((4,)),
            pltpu.SemaphoreType.DMA((owners,)),
            pltpu.SemaphoreType.DMA((owners,)),
        ],
        compiler_params=pltpu.CompilerParams(collective_id=0, has_side_effects=True),
    )(own, ghost_send, star_send)
    top = -(-rows // TILE)
    capacity = -(-(rows + 4 * wide) // TILE) * TILE + TILE
    spare = UNROLL + 4
    pairs = [(i, j) for j in range(top + 1) for i in range(j)]
    pairs = pairs + [(0, 0)] * spare
    first = jnp.asarray(np.array([a for a, _ in pairs], np.int32))
    second = jnp.asarray(np.array([b for _, b in pairs], np.int32))
    singles = (capacity // TILE) * top + spare + UNROLL
    return pl.pallas_call(
        functools.partial(gravity, sizes),
        out_shape=(
            jax.ShapeDtypeStruct((3, rows), F32),
            jax.ShapeDtypeStruct((4, rows), F32),
        ),
        in_specs=[smem] * 4 + [vmem] * 4 + [pl.BlockSpec(memory_space=pltpu.HBM)] * 5,
        out_specs=(vmem, vmem),
        scratch_shapes=[
            pltpu.VMEM((8, capacity), F32),
            pltpu.VMEM((capacity, FEATURES), BF16),
            pltpu.VMEM((FEATURES, capacity), BF16),
            pltpu.VMEM((16, capacity), BF16),
            pltpu.VMEM((16, capacity + TILE), F32),
            pltpu.VMEM((8, rows + 2 * TILE), F32),
            *square,
            pltpu.VMEM((2, LANES, FEATURES), BF16),
            pltpu.VMEM((2, FEATURES, LANES), BF16),
            pltpu.VMEM((2, LANES, LANES), F32),
            pltpu.VMEM((2, LANES, LANES), BF16),
            pltpu.VMEM((2, LANES, LANES), BF16),
            pltpu.VMEM((2, 16, LANES), BF16),
            pltpu.SMEM((leaves,), jnp.int32),
            pltpu.SMEM((singles,), jnp.int32),
            pltpu.SMEM((singles,), jnp.int32),
            pltpu.SMEM((slots + GROUP + 3,), jnp.int32),
            pltpu.SemaphoreType.DMA((5,)),
        ],
    )(
        leaf_counts, meta, first, second,
        own, gas_smoothing.reshape(leaves, LANES), ghost, star.reshape(slots, 8, LANES),
        *early,
    )


def solution(mesh):
    split = ("gx", "gy", "gz")
    placed = (
        P(None, split), P(split), P(split), P(split), P(split, None, None),
        P(None, split), P(split), P(None, split), P(split), P(split, None), P(split),
    )
    sizes = tuple(mesh.shape[axis] for axis in split)
    return jax.shard_map(
        functools.partial(on_device, sizes),
        mesh=mesh,
        in_specs=placed,
        out_specs=(P(None, split), P(None, split)),
        check_vma=False,
    )
```

```python
import functools
import math

import jax
import jax.numpy as jnp
import numpy as np
from jax import lax
from jax.experimental import pallas as pl
from jax.experimental.pallas import tpu as pltpu
from jax.sharding import PartitionSpec as P

LANES = 128
HALF = 64
CODE = 256
SLOTS = 3
SPLIT_SQ = 1.0
SOFT_SQ = 0.01
GRAVITY = 0.002
RADIAL_PUSH = 1.0

LOG2E = math.log2(math.e)
SCALE = LOG2E / (1.5 * SPLIT_SQ)
FACTOR = GRAVITY * math.exp(SOFT_SQ / SPLIT_SQ) * SCALE**1.5
MESH = pl.DeviceIdType.MESH
F32 = jnp.float32
BF16 = jnp.bfloat16

TILE = 256
FEATURES = 48
UNROLL = 8
GROUP = 8


def split3(x):
    a = x.astype(BF16).astype(F32)
    rest = x - a
    b = rest.astype(BF16).astype(F32)
    return a, b, rest - b


def nn(a, b):
    return jnp.dot(a, b, preferred_element_type=F32)


def nt(a, b):
    return lax.dot_general(a, b, (((1,), (1,)), ((), ())), preferred_element_type=F32)


def stack(parts):
    return jnp.concatenate(parts, axis=0)


def block_at(block):
    return pl.ds(pl.multiple_of(block * TILE, TILE), TILE)


def prepare_block(c, comp, side_a, side_b, weights, acc):
    here = block_at(c)
    sub = lax.broadcasted_iota(jnp.int32, (8, TILE), 0)
    tile = comp[:, here]
    u = tile - 0.5
    mass = tile[3:4]
    norm = SCALE * (u[0:1] * u[0:1] + u[1:2] * u[1:2] + u[2:3] * u[2:3])
    one = jnp.where(sub == 4, 1.0, 0.0)
    left = jnp.where(
        sub < 3, (-2.0 * SCALE) * u, jnp.where(sub == 3, norm + SCALE * SOFT_SQ, one)
    )
    p0, p1, p2 = split3(left)
    side_a[here, :] = stack([p0, p0, p1, p1, p0, p2]).T.astype(BF16)
    one = jnp.where(sub == 3, 1.0, 0.0)
    right = jnp.where(sub < 3, u, jnp.where(sub == 4, norm, one))
    q0, q1, q2 = split3(right)
    side_b[:, here] = stack([q0, q1, q0, q1, q2, q0]).astype(BF16)
    w0, w1, w2 = split3(jnp.where(sub < 3, mass * u, jnp.where(sub == 3, mass, 0.0)))
    w02 = jnp.where(sub < 4, w0, pltpu.roll(w2, 4, 0))
    weights[:, here] = stack([w02, w1]).astype(BF16)
    acc[:, here] = jnp.zeros((16, TILE), F32)


def distances(i, j, out, side_a, side_b):
    out[...] = nn(side_a[block_at(j), :], side_b[:, block_at(i)])


def kernel_values(d_ref, high, low):
    d = d_ref[...]
    value = jnp.exp2(-1.5 * (d + lax.log2(d)))
    h = value.astype(BF16)
    high[...] = h
    low[...] = (value - h.astype(F32)).astype(BF16)


def accumulate(i, j, to_i, to_j, high, low, weights, acc, both):
    h, l = high[...], low[...]
    w = weights[:, block_at(j)]
    acc[:, block_at(to_i)] = acc[:, block_at(to_i)] + (nn(w, h) + nn(w, l))
    if both:
        w = weights[:, block_at(i)]
        acc[:, block_at(to_j)] = acc[:, block_at(to_j)] + (nt(w, h) + nt(w, l))


def exchange(
    sizes,
    pos_ref, mass_ref, count_ref, ghost_ref,
    star_pos_ref, energy_ref, star_mom_ref, block_count_ref, owner_ref, leaf_ref,
    own, ghost_recv, star_recv, meta, comp, side_a, side_b, weights, acc,
    ghost_send, star_send, star_block, d0, d1, h0, h1, l0, l1,
    ghost_ssem, ghost_rsem, star_ssem, star_rsem,
):
    n_x, n_y, n_z, leaves, ghosts, blocks = sizes
    owners = n_y * n_z
    rows = leaves * LANES
    x, y, z = lax.axis_index("gx"), lax.axis_index("gy"), lax.axis_index("gz")
    me = y * n_z + z

    def owner_at(d):
        other = lax.rem(me + d, owners)
        return other, (x, lax.div(other, n_z), lax.rem(other, n_z))

    def beside(k):
        step = 1 if k % 2 == 0 else -1
        if k < 2:
            return (lax.rem(x + step + n_x, n_x), y, z)
        return (x, lax.rem(y + step + n_y, n_y), z)

    barrier = pltpu.get_barrier_semaphore()
    for k in range(2):
        pl.semaphore_signal(barrier, inc=1, device_id=beside(k), device_id_type=MESH)

    @pl.loop(1, owners)
    def _(d):
        pl.semaphore_signal(barrier, inc=1, device_id=owner_at(d)[1], device_id_type=MESH)

    lane = lax.broadcasted_iota(jnp.int32, (8, LANES), 1)
    row_lane = lane[0:1]

    def filled(scalar):
        return jnp.full((8, LANES), scalar)

    for b in range(blocks):
        here = slice(b * LANES, (b + 1) * LANES)
        live = row_lane < block_count_ref[b]
        star_block[b, 0:3] = star_pos_ref[:, here]
        star_block[b, 3:4] = jnp.where(live, energy_ref[b : b + 1, :], 0.0)
        star_block[b, 4:7] = jnp.where(live, star_mom_ref[:, here], 0.0)
        code = leaf_ref[b] * CODE + block_count_ref[b]
        star_block[b, 7:8] = filled(code)[0:1].astype(F32)

    @pl.loop(0, owners)
    def _(o):
        found = [jnp.zeros((8, LANES), F32)] * SLOTS
        for b in range(blocks):
            hit = filled(owner_ref[b]) == o
            tile = star_block[b]
            found = [jnp.where(hit, new, old) for new, old in zip([tile] + found, found)]
        for k in range(SLOTS):
            star_send[o, k] = found[k]

    own[0:3, :] = pos_ref[...]
    own[4:8, :] = jnp.zeros((4, rows), F32)
    for l in range(leaves):
        here = slice(l * LANES, (l + 1) * LANES)
        alive = row_lane < count_ref[l]
        own[3:4, here] = jnp.where(alive, mass_ref[l : l + 1, :], 0.0)
        own[7:8, here] = filled(count_ref[l])[0:1].astype(F32)
    for k in range(4):
        chosen = [filled(ghost_ref[g, k]) for g in range(ghosts)]
        picked = [own[:, 0:LANES]] * ghosts
        for l in range(1, leaves):
            tile = own[:, l * LANES : (l + 1) * LANES]
            picked = [jnp.where(c == l, tile, old) for c, old in zip(chosen, picked)]
        for g in range(ghosts):
            ghost_send[k, :, g * LANES : (g + 1) * LANES] = picked[g]
    for t in range(leaves // 2):
        left = own[:, 2 * t * LANES : (2 * t + 1) * LANES]
        right = own[:, (2 * t + 1) * LANES : (2 * t + 2) * LANES]
        comp[:, t * LANES : (t + 1) * LANES] = jnp.where(
            lane < HALF, left, pltpu.roll(right, HALF, 1)
        )

    pl.semaphore_wait(barrier, owners + 1)

    def ghost_copy(k):
        return pltpu.make_async_remote_copy(
            src_ref=ghost_send.at[k], dst_ref=ghost_recv.at[k],
            send_sem=ghost_ssem.at[k], recv_sem=ghost_rsem.at[k],
            device_id=beside(k), device_id_type=MESH,
        )

    def star_copy(d):
        other, where = owner_at(d)
        return pltpu.make_async_remote_copy(
            src_ref=star_send.at[other], dst_ref=star_recv.at[me],
            send_sem=star_ssem.at[d], recv_sem=star_rsem.at[d],
            device_id=where, device_id_type=MESH,
        )

    @pl.loop(1, owners)
    def _(d):
        star_copy(d).start()

    for k in range(4):
        ghost_copy(k).start()
    star_recv[me] = star_send[me]

    firm = comp.shape[1] // TILE

    @pl.loop(0, firm)
    def _(c):
        prepare_block(c, comp, side_a, side_b, weights, acc)

    distance, high, low = (d0, d1), (h0, h1), (l0, l1)

    period = firm + 1
    unroll = 2 * period
    assert firm % 4 == 0

    def task(g, e):
        g, e = g + e // unroll, e % unroll
        half, r = divmod(e, period)
        middle = (firm - 1) // 2
        if r in (middle, firm):
            i = (4 * g + 2 * half + r // firm) % firm
            return i, i, False
        p = (2 * g + half) * (firm - 1) + r - r // (middle + 1)
        i = p % firm
        return i, (i + 1 + p // firm) % firm, True

    distances(*task(0, 0)[:2], d0, side_a, side_b)
    distances(*task(0, 1)[:2], d1, side_a, side_b)
    kernel_values(d0, h0, l0)

    @pl.loop(0, firm // 4)
    def _(g):
        for e in range(unroll):
            even = e % 2
            i, j, both = task(g, e)
            distances(*task(g, e + 2)[:2], distance[even], side_a, side_b)
            kernel_values(distance[1 - even], high[1 - even], low[1 - even])
            accumulate(i, j, i, j, high[even], low[even], weights, acc, both)

    for k in range(4):
        ghost_copy(k).wait()

    @pl.loop(1, owners)
    def _(d):
        star_copy(d).wait()

    codes = [
        ghost_recv[k, 7:8, g * LANES : (g + 1) * LANES] for k in range(4) for g in range(ghosts)
    ]
    codes = codes + [star_recv[o, k, 7:8] for o in range(owners) for k in range(SLOTS)]
    for r in range(meta.shape[0]):
        line = jnp.zeros((1, LANES), F32)
        for e, code in enumerate(codes[r * LANES : (r + 1) * LANES]):
            line = jnp.where(row_lane == e, code, line)
        meta[r : r + 1, :] = line.astype(jnp.int32)


def gravity(
    sizes,
    count_ref, meta_ref, first_ref, second_ref,
    own_ref, smooth_ref, ghost_ref, star_ref,
    comp_in, a_in, b_in, weights_in, acc_in,
    accel_ref, deposit_ref,
    comp, side_a, side_b, weights, acc, res,
    d0, d1, h0, h1, l0, l1,
    star_a, star_b, star_d, star_h, star_l, star_v,
    offsets, slots, sems,
):
    n_x, n_y, n_z, leaves, ghosts, blocks = sizes
    owners = n_y * n_z
    rows = leaves * LANES
    capacity = comp.shape[1]
    trash = acc.shape[1] // TILE - 1
    lane = lax.broadcasted_iota(jnp.int32, (8, LANES), 1)
    sub = lax.broadcasted_iota(jnp.int32, (8, LANES), 0)
    settled = comp_in.shape[1]

    def meta_at(e):
        if meta_ref.shape[0] == 1:
            return meta_ref[0, e]
        return meta_ref[lax.div(e, LANES), lax.rem(e, LANES)]

    firm = settled // TILE

    copies = [
        pltpu.make_async_copy(comp_in, comp.at[:, 0:settled], sems.at[0]),
        pltpu.make_async_copy(a_in, side_a.at[0:settled, :], sems.at[1]),
        pltpu.make_async_copy(b_in, side_b.at[:, 0:settled], sems.at[2]),
        pltpu.make_async_copy(weights_in, weights.at[:, 0:settled], sems.at[3]),
        pltpu.make_async_copy(acc_in, acc.at[:, 0:settled], sems.at[4]),
    ]
    for copy in copies:
        copy.start()

    def place(tile, count, skip, off, current):
        turn = lax.rem(off, LANES)
        base = pl.multiple_of(off - turn, LANES)
        rolled = pltpu.roll(tile, lax.rem(turn + (LANES - skip), LANES), 1)
        current = jnp.where(lane >= turn, rolled, current)
        comp[:, pl.ds(base, LANES)] = current
        return off + count, jnp.where(turn + count >= LANES, rolled, current)

    def own_leaf(l, carry):
        offsets[l] = carry[0]
        start = pl.multiple_of(l * LANES, LANES)
        return place(own_ref[:, pl.ds(start, LANES)], count_ref[l] - HALF, HALF, *carry)

    carry = lax.fori_loop(
        0, leaves, own_leaf, (jnp.int32(settled), jnp.zeros((8, LANES), F32)), unroll=8
    )
    n_own = carry[0]
    for k in range(4):
        shift = jnp.where(sub == k // 2, -1.0 if k % 2 == 0 else 1.0, 0.0)
        for g in range(ghosts):
            tile = ghost_ref[k, :, g * LANES : (g + 1) * LANES] + shift
            count = meta_at(k * ghosts + g)
            carry = place(tile, count, 0, *carry)
    n_all, current = carry
    turn = lax.rem(n_all, LANES)
    base = n_all - turn
    comp[:, pl.ds(pl.multiple_of(base, LANES), LANES)] = jnp.where(lane < turn, current, 0.0)
    for extra in range(1, TILE // LANES):
        at = pl.multiple_of(base + extra * LANES, LANES)
        comp[:, pl.ds(at, LANES)] = jnp.zeros((8, LANES), F32)
    targets = lax.div(n_own + (TILE - 1), TILE)
    sources = lax.div(n_all + (TILE - 1), TILE)

    for copy in copies:
        copy.wait()

    def prepare(c, _):
        prepare_block(c, comp, side_a, side_b, weights, acc)
        return 0

    lax.fori_loop(firm, sources, prepare, 0)

    distance, high, low = (d0, d1), (h0, h1), (l0, l1)

    def tiles(kinds, unroll):
        steps = 0
        for _, begin, count, _ in kinds:
            steps = jnp.maximum(steps, len(kinds) * (count - begin) + 2)

        def entry(u, base, ahead):
            task, begin, count, both = kinds[(u + ahead) % len(kinds)]
            return task, begin, count, both, begin + base + (u + ahead) // len(kinds)

        def step(base, u):
            even = u % 2
            task, *_, k = entry(u, base, 0)
            distances(*task(k), distance[even], side_a, side_b)
            kernel_values(distance[1 - even], high[1 - even], low[1 - even])
            task, begin, count, both, k = entry(u, base, -2)
            valid = jnp.logical_and(k >= begin, k < count)
            i, j = task(jnp.maximum(k, begin))
            to_i, to_j = jnp.where(valid, i, trash), jnp.where(valid, j, trash)
            accumulate(i, j, to_i, to_j, high[even], low[even], weights, acc, both)

        @pl.loop(0, lax.div(steps + (unroll - 1), unroll))
        def _(g):
            for u in range(unroll):
                step(g * (unroll // len(kinds)), u)

    done = firm * (firm - 1) // 2
    n_both = lax.div(targets * (targets - 1), 2) - done
    squares = targets - firm
    n_one = squares + targets * (sources - targets)

    def both_task(k):
        return first_ref[done + k], second_ref[done + k]

    def one_task(k):
        past = k - squares
        column = lax.div(jnp.maximum(past, 0), targets)
        square = jnp.minimum(firm + k, targets - 1)
        i = jnp.where(past < 0, square, past - column * targets)
        j = jnp.where(past < 0, square, jnp.minimum(targets + column, sources - 1))
        return i, j

    tiles(
        [(both_task, 0, n_both, True), (one_task, 0, jnp.minimum(n_one, n_both), False)], UNROLL
    )

    @pl.when(n_one > n_both)
    def _():
        tiles([(one_task, n_both, n_one, False)], UNROLL // 2)

    def finish(c, _):
        here = block_at(c)
        head, tail = acc[0:8, here], acc[8:16, here]
        total = head + pltpu.roll(head, 4, 0) + tail
        res[:, here] = FACTOR * (total - (comp[:, here] - 0.5) * total[3:4])
        return 0

    lax.fori_loop(0, targets, finish, 0)

    def spread(l, side):
        off = offsets[l]
        turn = lax.rem(off, LANES)
        base = pl.multiple_of(off - turn, LANES)
        both = jnp.where(
            lane >= turn,
            res[:, pl.ds(base, LANES)],
            res[:, pl.ds(pl.multiple_of(base + LANES, LANES), LANES)],
        )
        back = pltpu.roll(both, lax.rem(LANES + HALF - turn, LANES), 1)
        back = jnp.where(lane < HALF, side, back)
        start = pl.multiple_of(l * LANES, LANES)
        accel_ref[:, pl.ds(start, LANES)] = jnp.where(lane < count_ref[l], back, 0.0)[0:3]
        deposit_ref[:, pl.ds(start, LANES)] = jnp.zeros((4, LANES), F32)

    def spread_two(t, _):
        side = res[:, pl.ds(pl.multiple_of(t * LANES, LANES), LANES)]
        spread(2 * t, side)
        spread(2 * t + 1, pltpu.roll(side, HALF, 1))
        return 0

    lax.fori_loop(0, leaves // 2, spread_two, 0, unroll=4)

    def valid_slot(s, n):
        slots[n] = s
        return n + jnp.where(lax.rem(meta_at(4 * ghosts + s), CODE) > 0, 1, 0)

    n_slots = lax.fori_loop(0, owners * SLOTS, valid_slot, jnp.int32(0), unroll=8)
    def empty_slot(e, _):
        slots[e] = 0
        return 0

    lax.fori_loop(n_slots, n_slots + GROUP + 3, empty_slot, 0)

    def slot_at(n):
        s = slots[n]
        leaf = lax.div(meta_at(4 * ghosts + s), CODE)
        there = pl.ds(pl.multiple_of(leaf * LANES, LANES), LANES)
        return star_ref[s], own_ref[:, there] - 0.5, leaf, there

    def star_features(n, left_out, right_out):
        star, gas, leaf, _ = slot_at(n)
        h = smooth_ref[pl.ds(leaf, 1), :]
        inverse = LOG2E / (h * h)
        ys = star - 0.5
        gas_norm = gas[0:1] * gas[0:1] + gas[1:2] * gas[1:2] + gas[2:3] * gas[2:3]
        star_norm = ys[0:1] * ys[0:1] + ys[1:2] * ys[1:2] + ys[2:3] * ys[2:3]
        left = jnp.where(
            sub < 3,
            (2.0 * inverse) * gas,
            jnp.where(sub == 3, -inverse * gas_norm, jnp.where(sub == 4, -inverse, 0.0)),
        )
        right = jnp.where(
            sub < 3, ys, jnp.where(sub == 3, 1.0, jnp.where(sub == 4, star_norm, 0.0))
        )
        p0, p1, p2 = split3(left)
        q0, q1, q2 = split3(right)
        left_out[...] = stack([p0, p0, p1, p1, p0, p2]).T.astype(BF16)
        right_out[...] = stack([q0, q1, q0, q1, q2, q0]).astype(BF16)

    def star_weights(n, exponent, high, low, value_out):
        weight = jnp.exp2(exponent[...])
        hi = weight.astype(BF16)
        high[...] = hi
        low[...] = (weight - hi.astype(F32)).astype(BF16)
        share = 1.0 / (1.0 + jnp.sum(weight, axis=0, keepdims=True))
        star = star_ref[slots[n]]
        energy = star[3:4]
        momentum = pltpu.roll(star, 4, 0)
        value = jnp.where(sub < 3, momentum - RADIAL_PUSH * energy * (star - 0.5), energy)
        v0, v1, v2 = split3(jnp.where(sub < 4, value * share, 0.0))
        v02 = jnp.where(sub < 4, v0, pltpu.roll(v2, 4, 0))
        value_out[...] = stack([v02, v1]).astype(BF16)

    def star_deposit(n, high, low, value):
        _, gas, leaf, there = slot_at(jnp.maximum(n, 0))
        v = value[...]
        out = nt(v, high[...]) + nt(v, low[...])
        head, tail = out[0:8], out[8:16]
        total = head + pltpu.roll(head, 4, 0) + tail
        heat_here = total[3:4]
        kick = pltpu.roll(total + RADIAL_PUSH * heat_here * gas, 1, 0)
        both = jnp.where(sub == 0, heat_here, kick)
        valid = jnp.logical_and(n >= 0, n < n_slots)
        live = jnp.where(valid, count_ref[leaf], 0)
        deposit_ref[:, there] = deposit_ref[:, there] + jnp.where(lane < live, both, 0.0)[0:4]

    @pl.loop(0, lax.div(n_slots + 3 + GROUP - 1, GROUP))
    def _(t):
        for e in range(GROUP):
            n, even = t * GROUP + e, e % 2
            star_features(n, star_a.at[even], star_b.at[even])
            star_d[even] = nn(star_a[1 - even], star_b[1 - even])
            star_weights(
                jnp.maximum(n - 2, 0), star_d.at[1 - even],
                star_h.at[1 - even], star_l.at[1 - even], star_v.at[1 - even],
            )
            star_deposit(n - 3, star_h.at[even], star_l.at[even], star_v.at[even])


def on_device(
    mesh_sizes,
    gas_position, gas_mass, gas_smoothing, leaf_counts, ghost_lists,
    star_position, star_energy, star_momentum, block_counts, block_owners, block_leaves,
):
    n_x, n_y, n_z = mesh_sizes
    leaves = leaf_counts.shape[0]
    blocks = block_counts.shape[0]
    ghosts = ghost_lists.shape[2]
    rows = leaves * LANES
    owners = n_y * n_z
    slots = owners * SLOTS
    wide = ghosts * LANES
    vmem = pl.BlockSpec(memory_space=pltpu.VMEM)
    smem = pl.BlockSpec(memory_space=pltpu.SMEM)
    sizes = (n_x, n_y, n_z, leaves, ghosts, blocks)
    settled = leaves * HALF
    square = [pltpu.VMEM((TILE, TILE), F32)] * 2 + [pltpu.VMEM((TILE, TILE), BF16)] * 4
    own, ghost, star, meta, *early = pl.pallas_call(
        functools.partial(exchange, sizes),
        out_shape=(
            jax.ShapeDtypeStruct((8, rows), F32),
            jax.ShapeDtypeStruct((4, 8, wide), F32),
            jax.ShapeDtypeStruct((owners, SLOTS, 8, LANES), F32),
            jax.ShapeDtypeStruct((-(-(4 * ghosts + slots) // LANES), LANES), jnp.int32),
            jax.ShapeDtypeStruct((8, settled), F32),
            jax.ShapeDtypeStruct((settled, FEATURES), BF16),
            jax.ShapeDtypeStruct((FEATURES, settled), BF16),
            jax.ShapeDtypeStruct((16, settled), BF16),
            jax.ShapeDtypeStruct((16, settled), F32),
        ),
        in_specs=[vmem, vmem, smem, smem, vmem, vmem, vmem, smem, smem, smem],
        out_specs=(vmem,) * 9,
        scratch_shapes=[
            pltpu.VMEM((4, 8, wide), F32),
            pltpu.VMEM((owners, SLOTS, 8, LANES), F32),
            pltpu.VMEM((blocks, 8, LANES), F32),
            *square,
            pltpu.SemaphoreType.DMA((4,)),
            pltpu.SemaphoreType.DMA((4,)),
            pltpu.SemaphoreType.DMA((owners,)),
            pltpu.SemaphoreType.DMA((owners,)),
        ],
        compiler_params=pltpu.CompilerParams(collective_id=0, has_side_effects=True),
    )(
        gas_position,
        gas_mass.reshape(leaves, LANES),
        leaf_counts,
        ghost_lists[0].T,
        star_position,
        star_energy.reshape(blocks, LANES),
        star_momentum,
        block_counts,
        block_owners.reshape(-1),
        block_leaves,
    )
    top = -(-rows // TILE)
    capacity = -(-(rows + 4 * wide) // TILE) * TILE + TILE
    spare = UNROLL + 4
    pairs = [(i, j) for j in range(top + 1) for i in range(j)]
    pairs = pairs + [(0, 0)] * spare
    first = jnp.asarray(np.array([a for a, _ in pairs], np.int32))
    second = jnp.asarray(np.array([b for _, b in pairs], np.int32))
    return pl.pallas_call(
        functools.partial(gravity, sizes),
        out_shape=(
            jax.ShapeDtypeStruct((3, rows), F32),
            jax.ShapeDtypeStruct((4, rows), F32),
        ),
        in_specs=[smem] * 4 + [vmem] * 4 + [pl.BlockSpec(memory_space=pltpu.HBM)] * 5,
        out_specs=(vmem, vmem),
        scratch_shapes=[
            pltpu.VMEM((8, capacity), F32),
            pltpu.VMEM((capacity, FEATURES), BF16),
            pltpu.VMEM((FEATURES, capacity), BF16),
            pltpu.VMEM((16, capacity), BF16),
            pltpu.VMEM((16, capacity + TILE), F32),
            pltpu.VMEM((8, rows + 2 * TILE), F32),
            *square,
            pltpu.VMEM((2, LANES, FEATURES), BF16),
            pltpu.VMEM((2, FEATURES, LANES), BF16),
            pltpu.VMEM((2, LANES, LANES), F32),
            pltpu.VMEM((2, LANES, LANES), BF16),
            pltpu.VMEM((2, LANES, LANES), BF16),
            pltpu.VMEM((2, 16, LANES), BF16),
            pltpu.SMEM((leaves,), jnp.int32),
            pltpu.SMEM((slots + GROUP + 3,), jnp.int32),
            pltpu.SemaphoreType.DMA((5,)),
        ],
    )(
        leaf_counts, meta, first, second,
        own, gas_smoothing.reshape(leaves, LANES), ghost, star.reshape(slots, 8, LANES),
        *early,
    )


def solution(mesh):
    split = ("gx", "gy", "gz")
    placed = (
        P(None, split), P(split), P(split), P(split), P(split, None, None),
        P(None, split), P(split), P(None, split), P(split), P(split, None), P(split),
    )
    sizes = tuple(mesh.shape[axis] for axis in split)
    return jax.shard_map(
        functools.partial(on_device, sizes),
        mesh=mesh,
        in_specs=placed,
        out_specs=(P(None, split), P(None, split)),
        check_vma=False,
    )
```

```python
import functools
import math

import jax
import jax.numpy as jnp
import numpy as np
from jax import lax
from jax.experimental import pallas as pl
from jax.experimental.pallas import tpu as pltpu
from jax.sharding import PartitionSpec as P

LANES = 128
HALF = 64
CODE = 256
SLOTS = 3
SPLIT_SQ = 1.0
SOFT_SQ = 0.01
GRAVITY = 0.002
RADIAL_PUSH = 1.0

LOG2E = math.log2(math.e)
SCALE = LOG2E / (1.5 * SPLIT_SQ)
FACTOR = GRAVITY * math.exp(SOFT_SQ / SPLIT_SQ) * SCALE**1.5
MESH = pl.DeviceIdType.MESH
F32 = jnp.float32
BF16 = jnp.bfloat16

TILE = 256
FEATURES = 48
UNROLL = 8
GROUP = 8


def split3(x):
    a = x.astype(BF16).astype(F32)
    rest = x - a
    b = rest.astype(BF16).astype(F32)
    return a, b, rest - b


def nn(a, b):
    return jnp.dot(a, b, preferred_element_type=F32)


def nt(a, b):
    return lax.dot_general(a, b, (((1,), (1,)), ((), ())), preferred_element_type=F32)


def stack(parts):
    return jnp.concatenate(parts, axis=0)


def block_at(block):
    return pl.ds(pl.multiple_of(block * TILE, TILE), TILE)


def prepare_block(c, comp, side_a, side_b, weights, acc):
    here = block_at(c)
    sub = lax.broadcasted_iota(jnp.int32, (8, TILE), 0)
    tile = comp[:, here]
    u = tile - 0.5
    mass = tile[3:4]
    norm = SCALE * (u[0:1] * u[0:1] + u[1:2] * u[1:2] + u[2:3] * u[2:3])
    one = jnp.where(sub == 4, 1.0, 0.0)
    left = jnp.where(
        sub < 3, (-2.0 * SCALE) * u, jnp.where(sub == 3, norm + SCALE * SOFT_SQ, one)
    )
    p0, p1, p2 = split3(left)
    side_a[here, :] = stack([p0, p0, p1, p1, p0, p2]).T.astype(BF16)
    one = jnp.where(sub == 3, 1.0, 0.0)
    right = jnp.where(sub < 3, u, jnp.where(sub == 4, norm, one))
    q0, q1, q2 = split3(right)
    side_b[:, here] = stack([q0, q1, q0, q1, q2, q0]).astype(BF16)
    w0, w1, w2 = split3(jnp.where(sub < 3, mass * u, jnp.where(sub == 3, mass, 0.0)))
    w02 = jnp.where(sub < 4, w0, pltpu.roll(w2, 4, 0))
    weights[:, here] = stack([w02, w1]).astype(BF16)
    acc[:, here] = jnp.zeros((16, TILE), F32)


def distances(i, j, out, side_a, side_b):
    out[...] = nn(side_a[block_at(j), :], side_b[:, block_at(i)])


def kernel_values(d_ref, high, low):
    d = d_ref[...]
    value = jnp.exp2(-1.5 * (d + lax.log2(d)))
    h = value.astype(BF16)
    high[...] = h
    low[...] = (value - h.astype(F32)).astype(BF16)


def accumulate(i, j, to_i, to_j, high, low, weights, acc, both):
    h, l = high[...], low[...]
    w = weights[:, block_at(j)]
    acc[:, block_at(to_i)] = acc[:, block_at(to_i)] + (nn(w, h) + nn(w, l))
    if both:
        w = weights[:, block_at(i)]
        acc[:, block_at(to_j)] = acc[:, block_at(to_j)] + (nt(w, h) + nt(w, l))


def exchange(
    sizes,
    pos_ref, mass_ref, count_ref, ghost_ref,
    star_pos_ref, energy_ref, star_mom_ref, block_count_ref, owner_ref, leaf_ref,
    own, ghost_recv, star_recv, meta, acc, comp_out, a_out, b_out, weights_out,
    comp, side_a, side_b, weights,
    ghost_send, star_send, star_block, d0, d1, h0, h1, l0, l1,
    ghost_ssem, ghost_rsem, star_ssem, star_rsem, early_sems,
):
    n_x, n_y, n_z, leaves, ghosts, blocks = sizes
    owners = n_y * n_z
    rows = leaves * LANES
    x, y, z = lax.axis_index("gx"), lax.axis_index("gy"), lax.axis_index("gz")
    me = y * n_z + z

    def owner_at(d):
        other = lax.rem(me + d, owners)
        return other, (x, lax.div(other, n_z), lax.rem(other, n_z))

    def beside(k):
        step = 1 if k % 2 == 0 else -1
        if k < 2:
            return (lax.rem(x + step + n_x, n_x), y, z)
        return (x, lax.rem(y + step + n_y, n_y), z)

    barrier = pltpu.get_barrier_semaphore()
    for k in range(2):
        pl.semaphore_signal(barrier, inc=1, device_id=beside(k), device_id_type=MESH)

    @pl.loop(1, owners)
    def _(d):
        pl.semaphore_signal(barrier, inc=1, device_id=owner_at(d)[1], device_id_type=MESH)

    lane = lax.broadcasted_iota(jnp.int32, (8, LANES), 1)
    row_lane = lane[0:1]

    def filled(scalar):
        return jnp.full((8, LANES), scalar)

    for b in range(blocks):
        here = slice(b * LANES, (b + 1) * LANES)
        live = row_lane < block_count_ref[b]
        star_block[b, 0:3] = star_pos_ref[:, here]
        star_block[b, 3:4] = jnp.where(live, energy_ref[b : b + 1, :], 0.0)
        star_block[b, 4:7] = jnp.where(live, star_mom_ref[:, here], 0.0)
        code = leaf_ref[b] * CODE + block_count_ref[b]
        star_block[b, 7:8] = filled(code)[0:1].astype(F32)

    @pl.loop(0, owners)
    def _(o):
        found = [jnp.zeros((8, LANES), F32)] * SLOTS
        for b in range(blocks):
            hit = filled(owner_ref[b]) == o
            tile = star_block[b]
            found = [jnp.where(hit, new, old) for new, old in zip([tile] + found, found)]
        for k in range(SLOTS):
            star_send[o, k] = found[k]

    own[0:3, :] = pos_ref[...]
    own[4:8, :] = jnp.zeros((4, rows), F32)
    for l in range(leaves):
        here = slice(l * LANES, (l + 1) * LANES)
        alive = row_lane < count_ref[l]
        own[3:4, here] = jnp.where(alive, mass_ref[l : l + 1, :], 0.0)
        own[7:8, here] = filled(count_ref[l])[0:1].astype(F32)
    for k in range(4):
        chosen = [filled(ghost_ref[g, k]) for g in range(ghosts)]
        picked = [own[:, 0:LANES]] * ghosts
        for l in range(1, leaves):
            tile = own[:, l * LANES : (l + 1) * LANES]
            picked = [jnp.where(c == l, tile, old) for c, old in zip(chosen, picked)]
        for g in range(ghosts):
            ghost_send[k, :, g * LANES : (g + 1) * LANES] = picked[g]
    for t in range(leaves // 2):
        left = own[:, 2 * t * LANES : (2 * t + 1) * LANES]
        right = own[:, (2 * t + 1) * LANES : (2 * t + 2) * LANES]
        comp[:, t * LANES : (t + 1) * LANES] = jnp.where(
            lane < HALF, left, pltpu.roll(right, HALF, 1)
        )

    pl.semaphore_wait(barrier, owners + 1)

    def ghost_copy(k):
        return pltpu.make_async_remote_copy(
            src_ref=ghost_send.at[k], dst_ref=ghost_recv.at[k],
            send_sem=ghost_ssem.at[k], recv_sem=ghost_rsem.at[k],
            device_id=beside(k), device_id_type=MESH,
        )

    def star_copy(d):
        other, where = owner_at(d)
        return pltpu.make_async_remote_copy(
            src_ref=star_send.at[other], dst_ref=star_recv.at[me],
            send_sem=star_ssem.at[d], recv_sem=star_rsem.at[d],
            device_id=where, device_id_type=MESH,
        )

    @pl.loop(1, owners)
    def _(d):
        star_copy(d).start()

    for k in range(4):
        ghost_copy(k).start()
    star_recv[me] = star_send[me]

    firm = comp.shape[1] // TILE

    @pl.loop(0, firm // 4)
    def _(t):
        for e in range(4):
            prepare_block(4 * t + e, comp, side_a, side_b, weights, acc)

    early = [
        pltpu.make_async_copy(a_ref, b_ref, early_sems.at[e])
        for e, (a_ref, b_ref) in enumerate(
            [(comp, comp_out), (side_a, a_out), (side_b, b_out), (weights, weights_out)]
        )
    ]
    for copy in early:
        copy.start()

    distance, high, low = (d0, d1), (h0, h1), (l0, l1)

    period = firm + 1
    unroll = 2 * period
    assert firm % 4 == 0

    def task(g, e):
        g, e = g + e // unroll, e % unroll
        half, r = divmod(e, period)
        middle = (firm - 1) // 2
        if r in (middle, firm):
            i = (4 * g + 2 * half + r // firm) % firm
            return i, i, False
        p = (2 * g + half) * (firm - 1) + r - r // (middle + 1)
        i = p % firm
        return i, (i + 1 + p // firm) % firm, True

    distances(*task(0, 0)[:2], d0, side_a, side_b)
    distances(*task(0, 1)[:2], d1, side_a, side_b)
    kernel_values(d0, h0, l0)

    @pl.loop(0, firm // 4)
    def _(g):
        for e in range(unroll):
            even = e % 2
            i, j, both = task(g, e)
            distances(*task(g, e + 2)[:2], distance[even], side_a, side_b)
            kernel_values(distance[1 - even], high[1 - even], low[1 - even])
            accumulate(i, j, i, j, high[even], low[even], weights, acc, both)

    for copy in early:
        copy.wait()
    for k in range(4):
        ghost_copy(k).wait()

    @pl.loop(1, owners)
    def _(d):
        star_copy(d).wait()

    codes = [
        ghost_recv[k, 7:8, g * LANES : (g + 1) * LANES] for k in range(4) for g in range(ghosts)
    ]
    codes = codes + [star_recv[o, k, 7:8] for o in range(owners) for k in range(SLOTS)]
    for r in range(meta.shape[0]):
        line = jnp.zeros((1, LANES), F32)
        for e, code in enumerate(codes[r * LANES : (r + 1) * LANES]):
            line = jnp.where(row_lane == e, code, line)
        meta[r : r + 1, :] = line.astype(jnp.int32)


def gravity(
    sizes,
    count_ref, meta_ref, first_ref, second_ref,
    own_ref, smooth_ref, ghost_ref, star_ref,
    acc_in, comp_in, a_in, b_in, weights_in,
    accel_ref, deposit_ref,
    comp, side_a, side_b, weights, acc, res,
    d0, d1, h0, h1, l0, l1,
    star_a, star_b, star_d, star_h, star_l, star_v,
    offsets, slots, sems,
):
    n_x, n_y, n_z, leaves, ghosts, blocks = sizes
    owners = n_y * n_z
    rows = leaves * LANES
    capacity = comp.shape[1]
    trash = acc.shape[1] // TILE - 1
    lane = lax.broadcasted_iota(jnp.int32, (8, LANES), 1)
    sub = lax.broadcasted_iota(jnp.int32, (8, LANES), 0)
    settled = comp_in.shape[1]

    def meta_at(e):
        if meta_ref.shape[0] == 1:
            return meta_ref[0, e]
        return meta_ref[lax.div(e, LANES), lax.rem(e, LANES)]

    firm = settled // TILE

    copies = [
        pltpu.make_async_copy(comp_in, comp.at[:, 0:settled], sems.at[0]),
        pltpu.make_async_copy(a_in, side_a.at[0:settled, :], sems.at[1]),
        pltpu.make_async_copy(b_in, side_b.at[:, 0:settled], sems.at[2]),
        pltpu.make_async_copy(weights_in, weights.at[:, 0:settled], sems.at[3]),
        pltpu.make_async_copy(acc_in, acc.at[:, 0:settled], sems.at[4]),
    ]
    for copy in copies:
        copy.start()

    def place(tile, count, skip, off, current):
        turn = lax.rem(off, LANES)
        base = pl.multiple_of(off - turn, LANES)
        rolled = pltpu.roll(tile, lax.rem(turn + (LANES - skip), LANES), 1)
        current = jnp.where(lane >= turn, rolled, current)
        comp[:, pl.ds(base, LANES)] = current
        return off + count, jnp.where(turn + count >= LANES, rolled, current)

    def own_leaf(l, carry):
        offsets[l] = carry[0]
        start = pl.multiple_of(l * LANES, LANES)
        return place(own_ref[:, pl.ds(start, LANES)], count_ref[l] - HALF, HALF, *carry)

    carry = lax.fori_loop(
        0, leaves, own_leaf, (jnp.int32(settled), jnp.zeros((8, LANES), F32)), unroll=8
    )
    n_own = carry[0]
    for k in range(4):
        shift = jnp.where(sub == k // 2, -1.0 if k % 2 == 0 else 1.0, 0.0)
        for g in range(ghosts):
            tile = ghost_ref[k, :, g * LANES : (g + 1) * LANES] + shift
            count = meta_at(k * ghosts + g)
            carry = place(tile, count, 0, *carry)
    n_all, current = carry
    turn = lax.rem(n_all, LANES)
    base = n_all - turn
    comp[:, pl.ds(pl.multiple_of(base, LANES), LANES)] = jnp.where(lane < turn, current, 0.0)
    for extra in range(1, TILE // LANES):
        at = pl.multiple_of(base + extra * LANES, LANES)
        comp[:, pl.ds(at, LANES)] = jnp.zeros((8, LANES), F32)
    targets = lax.div(n_own + (TILE - 1), TILE)
    sources = lax.div(n_all + (TILE - 1), TILE)

    @pl.loop(0, lax.div(sources - firm + 1, 2))
    def _(t):
        for e in range(2):
            prepare_block(firm + 2 * t + e, comp, side_a, side_b, weights, acc)

    for copy in copies:
        copy.wait()

    distance, high, low = (d0, d1), (h0, h1), (l0, l1)

    def tiles(kinds, unroll):
        steps = 0
        for _, begin, count, _ in kinds:
            steps = jnp.maximum(steps, len(kinds) * (count - begin) + 2)

        def entry(u, base, ahead):
            task, begin, count, both = kinds[(u + ahead) % len(kinds)]
            return task, begin, count, both, begin + base + (u + ahead) // len(kinds)

        def step(base, u):
            even = u % 2
            task, *_, k = entry(u, base, 0)
            distances(*task(k), distance[even], side_a, side_b)
            kernel_values(distance[1 - even], high[1 - even], low[1 - even])
            task, begin, count, both, k = entry(u, base, -2)
            valid = jnp.logical_and(k >= begin, k < count)
            i, j = task(jnp.maximum(k, begin))
            to_i, to_j = jnp.where(valid, i, trash), jnp.where(valid, j, trash)
            accumulate(i, j, to_i, to_j, high[even], low[even], weights, acc, both)

        @pl.loop(0, lax.div(steps + (unroll - 1), unroll))
        def _(g):
            for u in range(unroll):
                step(g * (unroll // len(kinds)), u)

    done = firm * (firm - 1) // 2
    n_both = lax.div(targets * (targets - 1), 2) - done
    squares = targets - firm
    n_one = squares + targets * (sources - targets)

    def both_task(k):
        return first_ref[done + k], second_ref[done + k]

    def one_task(k):
        past = k - squares
        column = lax.div(jnp.maximum(past, 0), targets)
        square = jnp.minimum(firm + k, targets - 1)
        i = jnp.where(past < 0, square, past - column * targets)
        j = jnp.where(past < 0, square, jnp.minimum(targets + column, sources - 1))
        return i, j

    tiles(
        [(both_task, 0, n_both, True), (one_task, 0, jnp.minimum(n_one, n_both), False)], UNROLL
    )

    @pl.when(n_one > n_both)
    def _():
        tiles([(one_task, n_both, n_one, False)], UNROLL // 2)

    def finish(c, _):
        here = block_at(c)
        head, tail = acc[0:8, here], acc[8:16, here]
        total = head + pltpu.roll(head, 4, 0) + tail
        res[:, here] = FACTOR * (total - (comp[:, here] - 0.5) * total[3:4])
        return 0

    lax.fori_loop(0, targets, finish, 0)

    def spread(l, side):
        off = offsets[l]
        turn = lax.rem(off, LANES)
        base = pl.multiple_of(off - turn, LANES)
        both = jnp.where(
            lane >= turn,
            res[:, pl.ds(base, LANES)],
            res[:, pl.ds(pl.multiple_of(base + LANES, LANES), LANES)],
        )
        back = pltpu.roll(both, lax.rem(LANES + HALF - turn, LANES), 1)
        back = jnp.where(lane < HALF, side, back)
        start = pl.multiple_of(l * LANES, LANES)
        accel_ref[:, pl.ds(start, LANES)] = jnp.where(lane < count_ref[l], back, 0.0)[0:3]
        deposit_ref[:, pl.ds(start, LANES)] = jnp.zeros((4, LANES), F32)

    def spread_two(t, _):
        side = res[:, pl.ds(pl.multiple_of(t * LANES, LANES), LANES)]
        spread(2 * t, side)
        spread(2 * t + 1, pltpu.roll(side, HALF, 1))
        return 0

    lax.fori_loop(0, leaves // 2, spread_two, 0, unroll=4)

    def valid_slot(s, n):
        slots[n] = s
        return n + jnp.where(lax.rem(meta_at(4 * ghosts + s), CODE) > 0, 1, 0)

    n_slots = lax.fori_loop(0, owners * SLOTS, valid_slot, jnp.int32(0), unroll=8)
    def empty_slot(e, _):
        slots[e] = 0
        return 0

    lax.fori_loop(n_slots, n_slots + GROUP + 3, empty_slot, 0)

    def slot_at(n):
        s = slots[n]
        leaf = lax.div(meta_at(4 * ghosts + s), CODE)
        there = pl.ds(pl.multiple_of(leaf * LANES, LANES), LANES)
        return star_ref[s], own_ref[:, there] - 0.5, leaf, there

    def star_features(n, left_out, right_out):
        star, gas, leaf, _ = slot_at(n)
        h = smooth_ref[pl.ds(leaf, 1), :]
        inverse = LOG2E / (h * h)
        ys = star - 0.5
        gas_norm = gas[0:1] * gas[0:1] + gas[1:2] * gas[1:2] + gas[2:3] * gas[2:3]
        star_norm = ys[0:1] * ys[0:1] + ys[1:2] * ys[1:2] + ys[2:3] * ys[2:3]
        left = jnp.where(
            sub < 3,
            (2.0 * inverse) * gas,
            jnp.where(sub == 3, -inverse * gas_norm, jnp.where(sub == 4, -inverse, 0.0)),
        )
        right = jnp.where(
            sub < 3, ys, jnp.where(sub == 3, 1.0, jnp.where(sub == 4, star_norm, 0.0))
        )
        p0, p1, p2 = split3(left)
        q0, q1, q2 = split3(right)
        left_out[...] = stack([p0, p0, p1, p1, p0, p2]).T.astype(BF16)
        right_out[...] = stack([q0, q1, q0, q1, q2, q0]).astype(BF16)

    def star_weights(n, exponent, high, low, value_out):
        weight = jnp.exp2(exponent[...])
        hi = weight.astype(BF16)
        high[...] = hi
        low[...] = (weight - hi.astype(F32)).astype(BF16)
        share = 1.0 / (1.0 + jnp.sum(weight, axis=0, keepdims=True))
        star = star_ref[slots[n]]
        energy = star[3:4]
        momentum = pltpu.roll(star, 4, 0)
        value = jnp.where(sub < 3, momentum - RADIAL_PUSH * energy * (star - 0.5), energy)
        v0, v1, v2 = split3(jnp.where(sub < 4, value * share, 0.0))
        v02 = jnp.where(sub < 4, v0, pltpu.roll(v2, 4, 0))
        value_out[...] = stack([v02, v1]).astype(BF16)

    def star_deposit(n, high, low, value):
        _, gas, leaf, there = slot_at(jnp.maximum(n, 0))
        v = value[...]
        out = nt(v, high[...]) + nt(v, low[...])
        head, tail = out[0:8], out[8:16]
        total = head + pltpu.roll(head, 4, 0) + tail
        heat_here = total[3:4]
        kick = pltpu.roll(total + RADIAL_PUSH * heat_here * gas, 1, 0)
        both = jnp.where(sub == 0, heat_here, kick)
        valid = jnp.logical_and(n >= 0, n < n_slots)
        live = jnp.where(valid, count_ref[leaf], 0)
        deposit_ref[:, there] = deposit_ref[:, there] + jnp.where(lane < live, both, 0.0)[0:4]

    @pl.loop(0, lax.div(n_slots + 3 + GROUP - 1, GROUP))
    def _(t):
        for e in range(GROUP):
            n, even = t * GROUP + e, e % 2
            star_features(n, star_a.at[even], star_b.at[even])
            star_d[even] = nn(star_a[1 - even], star_b[1 - even])
            star_weights(
                jnp.maximum(n - 2, 0), star_d.at[1 - even],
                star_h.at[1 - even], star_l.at[1 - even], star_v.at[1 - even],
            )
            star_deposit(n - 3, star_h.at[even], star_l.at[even], star_v.at[even])


def on_device(
    mesh_sizes,
    gas_position, gas_mass, gas_smoothing, leaf_counts, ghost_lists,
    star_position, star_energy, star_momentum, block_counts, block_owners, block_leaves,
):
    n_x, n_y, n_z = mesh_sizes
    leaves = leaf_counts.shape[0]
    blocks = block_counts.shape[0]
    ghosts = ghost_lists.shape[2]
    rows = leaves * LANES
    owners = n_y * n_z
    slots = owners * SLOTS
    wide = ghosts * LANES
    vmem = pl.BlockSpec(memory_space=pltpu.VMEM)
    smem = pl.BlockSpec(memory_space=pltpu.SMEM)
    hbm = pl.BlockSpec(memory_space=pltpu.HBM)
    sizes = (n_x, n_y, n_z, leaves, ghosts, blocks)
    settled = leaves * HALF
    square = [pltpu.VMEM((TILE, TILE), F32)] * 2 + [pltpu.VMEM((TILE, TILE), BF16)] * 4
    own, ghost, star, meta, *early = pl.pallas_call(
        functools.partial(exchange, sizes),
        out_shape=(
            jax.ShapeDtypeStruct((8, rows), F32),
            jax.ShapeDtypeStruct((4, 8, wide), F32),
            jax.ShapeDtypeStruct((owners, SLOTS, 8, LANES), F32),
            jax.ShapeDtypeStruct((-(-(4 * ghosts + slots) // LANES), LANES), jnp.int32),
            jax.ShapeDtypeStruct((16, settled), F32),
            jax.ShapeDtypeStruct((8, settled), F32),
            jax.ShapeDtypeStruct((settled, FEATURES), BF16),
            jax.ShapeDtypeStruct((FEATURES, settled), BF16),
            jax.ShapeDtypeStruct((16, settled), BF16),
        ),
        in_specs=[vmem, vmem, smem, smem, vmem, vmem, vmem, smem, smem, smem],
        out_specs=(vmem,) * 5 + (hbm,) * 4,
        scratch_shapes=[
            pltpu.VMEM((8, settled), F32),
            pltpu.VMEM((settled, FEATURES), BF16),
            pltpu.VMEM((FEATURES, settled), BF16),
            pltpu.VMEM((16, settled), BF16),
            pltpu.VMEM((4, 8, wide), F32),
            pltpu.VMEM((owners, SLOTS, 8, LANES), F32),
            pltpu.VMEM((blocks, 8, LANES), F32),
            *square,
            pltpu.SemaphoreType.DMA((4,)),
            pltpu.SemaphoreType.DMA((4,)),
            pltpu.SemaphoreType.DMA((owners,)),
            pltpu.SemaphoreType.DMA((owners,)),
            pltpu.SemaphoreType.DMA((4,)),
        ],
        compiler_params=pltpu.CompilerParams(
            collective_id=0, has_side_effects=True
        ),
    )(
        gas_position,
        gas_mass.reshape(leaves, LANES),
        leaf_counts,
        ghost_lists[0].T,
        star_position,
        star_energy.reshape(blocks, LANES),
        star_momentum,
        block_counts,
        block_owners.reshape(-1),
        block_leaves,
    )
    top = -(-rows // TILE)
    capacity = -(-(rows + 4 * wide) // TILE) * TILE + TILE
    spare = UNROLL + 4
    pairs = [(i, j) for j in range(top + 1) for i in range(j)]
    pairs = pairs + [(0, 0)] * spare
    first = jnp.asarray(np.array([a for a, _ in pairs], np.int32))
    second = jnp.asarray(np.array([b for _, b in pairs], np.int32))
    return pl.pallas_call(
        functools.partial(gravity, sizes),
        out_shape=(
            jax.ShapeDtypeStruct((3, rows), F32),
            jax.ShapeDtypeStruct((4, rows), F32),
        ),
        in_specs=[smem] * 4 + [vmem] * 4 + [hbm] * 5,
        out_specs=(vmem, vmem),
        scratch_shapes=[
            pltpu.VMEM((8, capacity), F32),
            pltpu.VMEM((capacity, FEATURES), BF16),
            pltpu.VMEM((FEATURES, capacity), BF16),
            pltpu.VMEM((16, capacity), BF16),
            pltpu.VMEM((16, capacity + TILE), F32),
            pltpu.VMEM((8, rows + 2 * TILE), F32),
            *square,
            pltpu.VMEM((2, LANES, FEATURES), BF16),
            pltpu.VMEM((2, FEATURES, LANES), BF16),
            pltpu.VMEM((2, LANES, LANES), F32),
            pltpu.VMEM((2, LANES, LANES), BF16),
            pltpu.VMEM((2, LANES, LANES), BF16),
            pltpu.VMEM((2, 16, LANES), BF16),
            pltpu.SMEM((leaves,), jnp.int32),
            pltpu.SMEM((slots + GROUP + 3,), jnp.int32),
            pltpu.SemaphoreType.DMA((5,)),
        ],
    )(
        leaf_counts, meta, first, second,
        own, gas_smoothing.reshape(leaves, LANES), ghost, star.reshape(slots, 8, LANES),
        *early,
    )


def solution(mesh):
    split = ("gx", "gy", "gz")
    placed = (
        P(None, split), P(split), P(split), P(split), P(split, None, None),
        P(None, split), P(split), P(None, split), P(split), P(split, None), P(split),
    )
    sizes = tuple(mesh.shape[axis] for axis in split)
    return jax.shard_map(
        functools.partial(on_device, sizes),
        mesh=mesh,
        in_specs=placed,
        out_specs=(P(None, split), P(None, split)),
        check_vma=False,
    )
```

```python
import functools
import math

import jax
import jax.numpy as jnp
import numpy as np
from jax import lax
from jax.experimental import pallas as pl
from jax.experimental.pallas import tpu as pltpu
from jax.sharding import PartitionSpec as P

LANES = 128
HALF = 64
CODE = 256
SLOTS = 3
SPLIT_SQ = 1.0
SOFT_SQ = 0.01
GRAVITY = 0.002
RADIAL_PUSH = 1.0

LOG2E = math.log2(math.e)
SCALE = LOG2E / (1.5 * SPLIT_SQ)
FACTOR = GRAVITY * math.exp(SOFT_SQ / SPLIT_SQ) * SCALE**1.5
MESH = pl.DeviceIdType.MESH
F32 = jnp.float32
BF16 = jnp.bfloat16

TILE = 256
FEATURES = 48
UNROLL = 12
GROUP = 8


def split3(x):
    a = x.astype(BF16).astype(F32)
    rest = x - a
    b = rest.astype(BF16).astype(F32)
    return a, b, rest - b


def nn(a, b):
    return jnp.dot(a, b, preferred_element_type=F32)


def nt(a, b):
    return lax.dot_general(a, b, (((1,), (1,)), ((), ())), preferred_element_type=F32)


def stack(parts):
    return jnp.concatenate(parts, axis=0)


def block_at(block):
    return pl.ds(pl.multiple_of(block * TILE, TILE), TILE)


def prepare_block(c, comp, side_a, side_b, weights, acc):
    here = block_at(c)
    sub = lax.broadcasted_iota(jnp.int32, (8, TILE), 0)
    tile = comp[:, here]
    u = tile - 0.5
    mass = tile[3:4]
    norm = SCALE * (u[0:1] * u[0:1] + u[1:2] * u[1:2] + u[2:3] * u[2:3])
    one = jnp.where(sub == 4, 1.0, 0.0)
    left = jnp.where(
        sub < 3, (-2.0 * SCALE) * u, jnp.where(sub == 3, norm + SCALE * SOFT_SQ, one)
    )
    p0, p1, p2 = split3(left)
    side_a[here, :] = stack([p0, p0, p1, p1, p0, p2]).T.astype(BF16)
    one = jnp.where(sub == 3, 1.0, 0.0)
    right = jnp.where(sub < 3, u, jnp.where(sub == 4, norm, one))
    q0, q1, q2 = split3(right)
    side_b[:, here] = stack([q0, q1, q0, q1, q2, q0]).astype(BF16)
    w0, w1, w2 = split3(jnp.where(sub < 3, mass * u, jnp.where(sub == 3, mass, 0.0)))
    w02 = jnp.where(sub < 4, w0, pltpu.roll(w2, 4, 0))
    weights[:, here] = stack([w02, w1]).astype(BF16)
    acc[:, here] = jnp.zeros((16, TILE), F32)


def distances(i, j, out, side_a, side_b):
    out[...] = nn(side_a[block_at(j), :], side_b[:, block_at(i)])


def kernel_values(d_ref, high, low):
    d = d_ref[...]
    value = jnp.exp2(-1.5 * (d + lax.log2(d)))
    h = value.astype(BF16)
    high[...] = h
    low[...] = (value - h.astype(F32)).astype(BF16)


def accumulate(i, j, to_i, to_j, high, low, weights, acc, both):
    h, l = high[...], low[...]
    w = weights[:, block_at(j)]
    acc[:, block_at(to_i)] = acc[:, block_at(to_i)] + (nn(w, h) + nn(w, l))
    if both:
        w = weights[:, block_at(i)]
        acc[:, block_at(to_j)] = acc[:, block_at(to_j)] + (nt(w, h) + nt(w, l))


def exchange(
    sizes,
    pos_ref, mass_ref, count_ref, ghost_ref,
    star_pos_ref, energy_ref, star_mom_ref, block_count_ref, owner_ref, leaf_ref,
    own, ghost_recv, star_recv, meta, acc, comp_out, a_out, b_out, weights_out,
    comp, side_a, side_b, weights,
    ghost_send, star_send, star_block, d0, d1, h0, h1, l0, l1,
    ghost_ssem, ghost_rsem, star_ssem, star_rsem, early_sems,
):
    n_x, n_y, n_z, leaves, ghosts, blocks = sizes
    owners = n_y * n_z
    rows = leaves * LANES
    x, y, z = lax.axis_index("gx"), lax.axis_index("gy"), lax.axis_index("gz")
    me = y * n_z + z

    def owner_at(d):
        other = lax.rem(me + d, owners)
        return other, (x, lax.div(other, n_z), lax.rem(other, n_z))

    def beside(k):
        step = 1 if k % 2 == 0 else -1
        if k < 2:
            return (lax.rem(x + step + n_x, n_x), y, z)
        return (x, lax.rem(y + step + n_y, n_y), z)

    barrier = pltpu.get_barrier_semaphore()
    for k in range(2):
        pl.semaphore_signal(barrier, inc=1, device_id=beside(k), device_id_type=MESH)

    @pl.loop(1, owners)
    def _(d):
        pl.semaphore_signal(barrier, inc=1, device_id=owner_at(d)[1], device_id_type=MESH)

    lane = lax.broadcasted_iota(jnp.int32, (8, LANES), 1)
    row_lane = lane[0:1]

    def filled(scalar):
        return jnp.full((8, LANES), scalar)

    for b in range(blocks):
        here = slice(b * LANES, (b + 1) * LANES)
        live = row_lane < block_count_ref[b]
        star_block[b, 0:3] = star_pos_ref[:, here]
        star_block[b, 3:4] = jnp.where(live, energy_ref[b : b + 1, :], 0.0)
        star_block[b, 4:7] = jnp.where(live, star_mom_ref[:, here], 0.0)
        code = leaf_ref[b] * CODE + block_count_ref[b]
        star_block[b, 7:8] = filled(code)[0:1].astype(F32)

    @pl.loop(0, owners)
    def _(o):
        found = [jnp.zeros((8, LANES), F32)] * SLOTS
        for b in range(blocks):
            hit = filled(owner_ref[b]) == o
            tile = star_block[b]
            found = [jnp.where(hit, new, old) for new, old in zip([tile] + found, found)]
        for k in range(SLOTS):
            star_send[o, k] = found[k]

    own[0:3, :] = pos_ref[...]
    own[4:8, :] = jnp.zeros((4, rows), F32)
    for l in range(leaves):
        here = slice(l * LANES, (l + 1) * LANES)
        alive = row_lane < count_ref[l]
        own[3:4, here] = jnp.where(alive, mass_ref[l : l + 1, :], 0.0)
        own[7:8, here] = filled(count_ref[l])[0:1].astype(F32)
    for k in range(4):
        chosen = [filled(ghost_ref[g, k]) for g in range(ghosts)]
        picked = [own[:, 0:LANES]] * ghosts
        for l in range(1, leaves):
            tile = own[:, l * LANES : (l + 1) * LANES]
            picked = [jnp.where(c == l, tile, old) for c, old in zip(chosen, picked)]
        for g in range(ghosts):
            ghost_send[k, :, g * LANES : (g + 1) * LANES] = picked[g]
    for t in range(leaves // 2):
        left = own[:, 2 * t * LANES : (2 * t + 1) * LANES]
        right = own[:, (2 * t + 1) * LANES : (2 * t + 2) * LANES]
        comp[:, t * LANES : (t + 1) * LANES] = jnp.where(
            lane < HALF, left, pltpu.roll(right, HALF, 1)
        )

    pl.semaphore_wait(barrier, owners + 1)

    def ghost_copy(k):
        return pltpu.make_async_remote_copy(
            src_ref=ghost_send.at[k], dst_ref=ghost_recv.at[k],
            send_sem=ghost_ssem.at[k], recv_sem=ghost_rsem.at[k],
            device_id=beside(k), device_id_type=MESH,
        )

    def star_copy(d):
        other, where = owner_at(d)
        return pltpu.make_async_remote_copy(
            src_ref=star_send.at[other], dst_ref=star_recv.at[me],
            send_sem=star_ssem.at[d], recv_sem=star_rsem.at[d],
            device_id=where, device_id_type=MESH,
        )

    @pl.loop(1, owners)
    def _(d):
        star_copy(d).start()

    for k in range(4):
        ghost_copy(k).start()
    star_recv[me] = star_send[me]

    firm = comp.shape[1] // TILE

    @pl.loop(0, firm // 4)
    def _(t):
        for e in range(4):
            prepare_block(4 * t + e, comp, side_a, side_b, weights, acc)

    early = [
        pltpu.make_async_copy(a_ref, b_ref, early_sems.at[e])
        for e, (a_ref, b_ref) in enumerate(
            [(comp, comp_out), (side_a, a_out), (side_b, b_out), (weights, weights_out)]
        )
    ]
    for copy in early:
        copy.start()

    distance, high, low = (d0, d1), (h0, h1), (l0, l1)

    period = firm + 1
    unroll = 2 * period
    assert firm % 4 == 0

    def task(g, e):
        g, e = g + e // unroll, e % unroll
        half, r = divmod(e, period)
        middle = (firm - 1) // 2
        if r in (middle, firm):
            i = (4 * g + 2 * half + r // firm) % firm
            return i, i, False
        p = (2 * g + half) * (firm - 1) + r - r // (middle + 1)
        i = p % firm
        return i, (i + 1 + p // firm) % firm, True

    distances(*task(0, 0)[:2], d0, side_a, side_b)
    distances(*task(0, 1)[:2], d1, side_a, side_b)
    kernel_values(d0, h0, l0)

    @pl.loop(0, firm // 4)
    def _(g):
        for e in range(unroll):
            even = e % 2
            i, j, both = task(g, e)
            distances(*task(g, e + 2)[:2], distance[even], side_a, side_b)
            kernel_values(distance[1 - even], high[1 - even], low[1 - even])
            accumulate(i, j, i, j, high[even], low[even], weights, acc, both)

    for copy in early:
        copy.wait()
    for k in range(4):
        ghost_copy(k).wait()

    @pl.loop(1, owners)
    def _(d):
        star_copy(d).wait()

    codes = [
        ghost_recv[k, 7:8, g * LANES : (g + 1) * LANES] for k in range(4) for g in range(ghosts)
    ]
    codes = codes + [star_recv[o, k, 7:8] for o in range(owners) for k in range(SLOTS)]
    for r in range(meta.shape[0]):
        line = jnp.zeros((1, LANES), F32)
        for e, code in enumerate(codes[r * LANES : (r + 1) * LANES]):
            line = jnp.where(row_lane == e, code, line)
        meta[r : r + 1, :] = line.astype(jnp.int32)


def gravity(
    sizes,
    count_ref, meta_ref, first_ref, second_ref,
    own_ref, smooth_ref, ghost_ref, star_ref,
    acc_in, comp_in, a_in, b_in, weights_in,
    accel_ref, deposit_ref,
    comp, side_a, side_b, weights, acc, res,
    d0, d1, h0, h1, l0, l1,
    star_a, star_b, star_d, star_h, star_l, star_v,
    offsets, slots, sems,
):
    n_x, n_y, n_z, leaves, ghosts, blocks = sizes
    owners = n_y * n_z
    rows = leaves * LANES
    capacity = comp.shape[1]
    trash = acc.shape[1] // TILE - 1
    lane = lax.broadcasted_iota(jnp.int32, (8, LANES), 1)
    sub = lax.broadcasted_iota(jnp.int32, (8, LANES), 0)
    settled = comp_in.shape[1]

    def meta_at(e):
        if meta_ref.shape[0] == 1:
            return meta_ref[0, e]
        return meta_ref[lax.div(e, LANES), lax.rem(e, LANES)]

    firm = settled // TILE

    copies = [
        pltpu.make_async_copy(comp_in, comp.at[:, 0:settled], sems.at[0]),
        pltpu.make_async_copy(a_in, side_a.at[0:settled, :], sems.at[1]),
        pltpu.make_async_copy(b_in, side_b.at[:, 0:settled], sems.at[2]),
        pltpu.make_async_copy(weights_in, weights.at[:, 0:settled], sems.at[3]),
        pltpu.make_async_copy(acc_in, acc.at[:, 0:settled], sems.at[4]),
    ]
    for copy in copies:
        copy.start()

    def place(tile, count, skip, off, current):
        turn = off & (LANES - 1)
        base = pl.multiple_of(off - turn, LANES)
        rolled = pltpu.roll(tile, (turn + (LANES - skip)) & (LANES - 1), 1)
        current = jnp.where(lane >= turn, rolled, current)
        comp[:, pl.ds(base, LANES)] = current
        return off + count, jnp.where(turn + count >= LANES, rolled, current)

    def own_leaf(l, carry):
        offsets[l] = carry[0]
        start = pl.multiple_of(l * LANES, LANES)
        return place(own_ref[:, pl.ds(start, LANES)], count_ref[l] - HALF, HALF, *carry)

    carry = lax.fori_loop(
        0, leaves, own_leaf, (jnp.int32(settled), jnp.zeros((8, LANES), F32)), unroll=16
    )
    n_own = carry[0]
    for k in range(4):
        shift = jnp.where(sub == k // 2, -1.0 if k % 2 == 0 else 1.0, 0.0)
        for g in range(ghosts):
            tile = ghost_ref[k, :, g * LANES : (g + 1) * LANES] + shift
            count = meta_at(k * ghosts + g)
            carry = place(tile, count, 0, *carry)
    n_all, current = carry
    turn = n_all & (LANES - 1)
    base = n_all - turn
    comp[:, pl.ds(pl.multiple_of(base, LANES), LANES)] = jnp.where(lane < turn, current, 0.0)
    for extra in range(1, TILE // LANES):
        at = pl.multiple_of(base + extra * LANES, LANES)
        comp[:, pl.ds(at, LANES)] = jnp.zeros((8, LANES), F32)
    targets = lax.div(n_own + (TILE - 1), TILE)
    sources = lax.div(n_all + (TILE - 1), TILE)

    @pl.loop(0, lax.div(sources - firm + 1, 2))
    def _(t):
        for e in range(2):
            prepare_block(firm + 2 * t + e, comp, side_a, side_b, weights, acc)

    for copy in copies:
        copy.wait()

    distance, high, low = (d0, d1), (h0, h1), (l0, l1)

    def tiles(kinds, unroll):
        steps = 0
        for _, begin, count, _ in kinds:
            steps = jnp.maximum(steps, len(kinds) * (count - begin) + 2)

        def entry(u, base, ahead):
            task, begin, count, both = kinds[(u + ahead) % len(kinds)]
            return task, begin, count, both, begin + base + (u + ahead) // len(kinds)

        def step(base, u):
            even = u % 2
            task, *_, k = entry(u, base, 0)
            distances(*task(k), distance[even], side_a, side_b)
            kernel_values(distance[1 - even], high[1 - even], low[1 - even])
            task, begin, count, both, k = entry(u, base, -2)
            valid = jnp.logical_and(k >= begin, k < count)
            i, j = task(jnp.maximum(k, begin))
            to_i, to_j = jnp.where(valid, i, trash), jnp.where(valid, j, trash)
            accumulate(i, j, to_i, to_j, high[even], low[even], weights, acc, both)

        @pl.loop(0, lax.div(steps + (unroll - 1), unroll))
        def _(g):
            for u in range(unroll):
                step(g * (unroll // len(kinds)), u)

    done = firm * (firm - 1) // 2
    n_both = lax.div(targets * (targets - 1), 2) - done
    squares = targets - firm
    n_one = squares + targets * (sources - targets)

    def both_task(k):
        return first_ref[done + k], second_ref[done + k]

    def one_task(k):
        past = k - squares
        column = lax.div(jnp.maximum(past, 0), targets)
        square = jnp.minimum(firm + k, targets - 1)
        i = jnp.where(past < 0, square, past - column * targets)
        j = jnp.where(past < 0, square, jnp.minimum(targets + column, sources - 1))
        return i, j

    tiles(
        [(both_task, 0, n_both, True), (one_task, 0, jnp.minimum(n_one, n_both), False)], UNROLL
    )

    @pl.when(n_one > n_both)
    def _():
        tiles([(one_task, n_both, n_one, False)], UNROLL // 2)

    def finish(c):
        here = block_at(c)
        head, tail = acc[0:8, here], acc[8:16, here]
        total = head + pltpu.roll(head, 4, 0) + tail
        res[:, here] = FACTOR * (total - (comp[:, here] - 0.5) * total[3:4])

    @pl.loop(0, lax.div(targets + 3, 4))
    def _(t):
        for e in range(4):
            finish(4 * t + e)

    def spread(l, side):
        off = offsets[l]
        turn = off & (LANES - 1)
        base = pl.multiple_of(off - turn, LANES)
        both = jnp.where(
            lane >= turn,
            res[:, pl.ds(base, LANES)],
            res[:, pl.ds(pl.multiple_of(base + LANES, LANES), LANES)],
        )
        back = pltpu.roll(both, (LANES + HALF - turn) & (LANES - 1), 1)
        back = jnp.where(lane < HALF, side, back)
        start = pl.multiple_of(l * LANES, LANES)
        accel_ref[:, pl.ds(start, LANES)] = jnp.where(lane < count_ref[l], back, 0.0)[0:3]
        deposit_ref[:, pl.ds(start, LANES)] = jnp.zeros((4, LANES), F32)

    def spread_two(t, _):
        side = res[:, pl.ds(pl.multiple_of(t * LANES, LANES), LANES)]
        spread(2 * t, side)
        spread(2 * t + 1, pltpu.roll(side, HALF, 1))
        return 0

    lax.fori_loop(0, leaves // 2, spread_two, 0, unroll=8)

    def valid_slot(s, n):
        slots[n] = s
        return n + jnp.where(lax.rem(meta_at(4 * ghosts + s), CODE) > 0, 1, 0)

    n_slots = lax.fori_loop(0, owners * SLOTS, valid_slot, jnp.int32(0), unroll=8)
    def empty_slot(e, _):
        slots[e] = 0
        return 0

    lax.fori_loop(n_slots, n_slots + GROUP + 3, empty_slot, 0)

    def slot_at(n):
        s = slots[n]
        leaf = lax.div(meta_at(4 * ghosts + s), CODE)
        there = pl.ds(pl.multiple_of(leaf * LANES, LANES), LANES)
        return star_ref[s], own_ref[:, there] - 0.5, leaf, there

    def star_features(n, left_out, right_out):
        star, gas, leaf, _ = slot_at(n)
        h = smooth_ref[pl.ds(leaf, 1), :]
        inverse = LOG2E / (h * h)
        ys = star - 0.5
        gas_norm = gas[0:1] * gas[0:1] + gas[1:2] * gas[1:2] + gas[2:3] * gas[2:3]
        star_norm = ys[0:1] * ys[0:1] + ys[1:2] * ys[1:2] + ys[2:3] * ys[2:3]
        left = jnp.where(
            sub < 3,
            (2.0 * inverse) * gas,
            jnp.where(sub == 3, -inverse * gas_norm, jnp.where(sub == 4, -inverse, 0.0)),
        )
        right = jnp.where(
            sub < 3, ys, jnp.where(sub == 3, 1.0, jnp.where(sub == 4, star_norm, 0.0))
        )
        p0, p1, p2 = split3(left)
        q0, q1, q2 = split3(right)
        left_out[...] = stack([p0, p0, p1, p1, p0, p2]).T.astype(BF16)
        right_out[...] = stack([q0, q1, q0, q1, q2, q0]).astype(BF16)

    def star_weights(n, exponent, high, low, value_out):
        weight = jnp.exp2(exponent[...])
        hi = weight.astype(BF16)
        high[...] = hi
        low[...] = (weight - hi.astype(F32)).astype(BF16)
        share = 1.0 / (1.0 + jnp.sum(weight, axis=0, keepdims=True))
        star = star_ref[slots[n]]
        energy = star[3:4]
        momentum = pltpu.roll(star, 4, 0)
        value = jnp.where(sub < 3, momentum - RADIAL_PUSH * energy * (star - 0.5), energy)
        v0, v1, v2 = split3(jnp.where(sub < 4, value * share, 0.0))
        v02 = jnp.where(sub < 4, v0, pltpu.roll(v2, 4, 0))
        value_out[...] = stack([v02, v1]).astype(BF16)

    def star_deposit(n, high, low, value):
        _, gas, leaf, there = slot_at(jnp.maximum(n, 0))
        v = value[...]
        out = nt(v, high[...]) + nt(v, low[...])
        head, tail = out[0:8], out[8:16]
        total = head + pltpu.roll(head, 4, 0) + tail
        heat_here = total[3:4]
        kick = pltpu.roll(total + RADIAL_PUSH * heat_here * gas, 1, 0)
        both = jnp.where(sub == 0, heat_here, kick)
        valid = jnp.logical_and(n >= 0, n < n_slots)
        live = jnp.where(valid, count_ref[leaf], 0)
        deposit_ref[:, there] = deposit_ref[:, there] + jnp.where(lane < live, both, 0.0)[0:4]

    @pl.loop(0, lax.div(n_slots + 3 + GROUP - 1, GROUP))
    def _(t):
        for e in range(GROUP):
            n, even = t * GROUP + e, e % 2
            star_features(n, star_a.at[even], star_b.at[even])
            star_d[even] = nn(star_a[1 - even], star_b[1 - even])
            star_weights(
                jnp.maximum(n - 2, 0), star_d.at[1 - even],
                star_h.at[1 - even], star_l.at[1 - even], star_v.at[1 - even],
            )
            star_deposit(n - 3, star_h.at[even], star_l.at[even], star_v.at[even])


def on_device(
    mesh_sizes,
    gas_position, gas_mass, gas_smoothing, leaf_counts, ghost_lists,
    star_position, star_energy, star_momentum, block_counts, block_owners, block_leaves,
):
    n_x, n_y, n_z = mesh_sizes
    leaves = leaf_counts.shape[0]
    blocks = block_counts.shape[0]
    ghosts = ghost_lists.shape[2]
    rows = leaves * LANES
    owners = n_y * n_z
    slots = owners * SLOTS
    wide = ghosts * LANES
    vmem = pl.BlockSpec(memory_space=pltpu.VMEM)
    smem = pl.BlockSpec(memory_space=pltpu.SMEM)
    hbm = pl.BlockSpec(memory_space=pltpu.HBM)
    sizes = (n_x, n_y, n_z, leaves, ghosts, blocks)
    settled = leaves * HALF
    square = [pltpu.VMEM((TILE, TILE), F32)] * 2 + [pltpu.VMEM((TILE, TILE), BF16)] * 4
    own, ghost, star, meta, *early = pl.pallas_call(
        functools.partial(exchange, sizes),
        out_shape=(
            jax.ShapeDtypeStruct((8, rows), F32),
            jax.ShapeDtypeStruct((4, 8, wide), F32),
            jax.ShapeDtypeStruct((owners, SLOTS, 8, LANES), F32),
            jax.ShapeDtypeStruct((-(-(4 * ghosts + slots) // LANES), LANES), jnp.int32),
            jax.ShapeDtypeStruct((16, settled), F32),
            jax.ShapeDtypeStruct((8, settled), F32),
            jax.ShapeDtypeStruct((settled, FEATURES), BF16),
            jax.ShapeDtypeStruct((FEATURES, settled), BF16),
            jax.ShapeDtypeStruct((16, settled), BF16),
        ),
        in_specs=[vmem, vmem, smem, smem, vmem, vmem, vmem, smem, smem, smem],
        out_specs=(vmem,) * 5 + (hbm,) * 4,
        scratch_shapes=[
            pltpu.VMEM((8, settled), F32),
            pltpu.VMEM((settled, FEATURES), BF16),
            pltpu.VMEM((FEATURES, settled), BF16),
            pltpu.VMEM((16, settled), BF16),
            pltpu.VMEM((4, 8, wide), F32),
            pltpu.VMEM((owners, SLOTS, 8, LANES), F32),
            pltpu.VMEM((blocks, 8, LANES), F32),
            *square,
            pltpu.SemaphoreType.DMA((4,)),
            pltpu.SemaphoreType.DMA((4,)),
            pltpu.SemaphoreType.DMA((owners,)),
            pltpu.SemaphoreType.DMA((owners,)),
            pltpu.SemaphoreType.DMA((4,)),
        ],
        compiler_params=pltpu.CompilerParams(
            collective_id=0, has_side_effects=True
        ),
    )(
        gas_position,
        gas_mass.reshape(leaves, LANES),
        leaf_counts,
        ghost_lists[0].T,
        star_position,
        star_energy.reshape(blocks, LANES),
        star_momentum,
        block_counts,
        block_owners.reshape(-1),
        block_leaves,
    )
    top = -(-rows // TILE)
    capacity = -(-(rows + 4 * wide) // TILE) * TILE + TILE
    spare = UNROLL + 4
    pairs = [(i, j) for j in range(top + 1) for i in range(j)]
    pairs = pairs + [(0, 0)] * spare
    first = jnp.asarray(np.array([a for a, _ in pairs], np.int32))
    second = jnp.asarray(np.array([b for _, b in pairs], np.int32))
    return pl.pallas_call(
        functools.partial(gravity, sizes),
        out_shape=(
            jax.ShapeDtypeStruct((3, rows), F32),
            jax.ShapeDtypeStruct((4, rows), F32),
        ),
        in_specs=[smem] * 4 + [vmem] * 4 + [hbm] * 5,
        out_specs=(vmem, vmem),
        scratch_shapes=[
            pltpu.VMEM((8, capacity), F32),
            pltpu.VMEM((capacity, FEATURES), BF16),
            pltpu.VMEM((FEATURES, capacity), BF16),
            pltpu.VMEM((16, capacity), BF16),
            pltpu.VMEM((16, capacity + TILE), F32),
            pltpu.VMEM((8, rows + 4 * TILE), F32),
            *square,
            pltpu.VMEM((2, LANES, FEATURES), BF16),
            pltpu.VMEM((2, FEATURES, LANES), BF16),
            pltpu.VMEM((2, LANES, LANES), F32),
            pltpu.VMEM((2, LANES, LANES), BF16),
            pltpu.VMEM((2, LANES, LANES), BF16),
            pltpu.VMEM((2, 16, LANES), BF16),
            pltpu.SMEM((leaves,), jnp.int32),
            pltpu.SMEM((slots + GROUP + 3,), jnp.int32),
            pltpu.SemaphoreType.DMA((5,)),
        ],
    )(
        leaf_counts, meta, first, second,
        own, gas_smoothing.reshape(leaves, LANES), ghost, star.reshape(slots, 8, LANES),
        *early,
    )


def solution(mesh):
    split = ("gx", "gy", "gz")
    placed = (
        P(None, split), P(split), P(split), P(split), P(split, None, None),
        P(None, split), P(split), P(None, split), P(split), P(split, None), P(split),
    )
    sizes = tuple(mesh.shape[axis] for axis in split)
    return jax.shard_map(
        functools.partial(on_device, sizes),
        mesh=mesh,
        in_specs=placed,
        out_specs=(P(None, split), P(None, split)),
        check_vma=False,
    )
```
